256 devices in a mesh: cells: 64 (over z, y, core), genes: 4 (over x).
Axes of the slice: x: 4, y: 4, z: 8, core: 2. Of those that a mesh axis runs over, the one named last changes fastest.
Arguments:
- counts: int32 [8192, 33280], P('cells', 'genes'), may hold values from 0 to 64, as said below
- live_rows: int32 [64], P('cells'), may hold values from 64 to 128, as said below
- left_basis: float32 [32, 8192], P(None, 'cells'), may hold values from -0.0625 to 0.0625
- right_basis: float32 [32, 33280], P(None, 'genes'), may hold values from -0.03125 to 0.03125
- right_start: float32 [16, 33280], P(None, 'genes'), may hold values from -0.03125 to 0.03125
Outputs:
- left_vectors: float32 [48, 8192], P(None, 'cells')
- right_vectors: float32 [48, 33280], P(None, 'genes')
- diag_blocks: float32 [3, 16, 16], replicated
- couple_blocks: float32 [3, 16, 16], replicated
The draws below stay inside these ranges and needn't reach their ends.
Inputs may be any that keep to these rules, and one draw needn't show every extreme that they name: `counts`: rows of a cell block at or beyond its live count are padding and are not part of the matrix. `live_rows`: entry b is the number of live rows, the first ones, of cell block b; some block is full in every draw.
All inputs are finite; a program needn't handle non-finite values.
Results may differ from the reference program's by a relative error of at most 0.0003.
Values sent between devices are 32-bit elements; how exact they have to be, the bound alone decides.
No kernel may reach another device: no remote copies, remote signals or barrier semaphores. Data moves between devices by JAX's collectives and lax.ppermute only.
A program may use at most 64 MiB of HBM per device.

```python
import jax
import jax.numpy as jnp
from jax import lax

CELL_DEV = 128
GENES = 33280
BASIS = 32
BLOCK = 16
STEPS = 3
CELL_BLOCKS = 64
CELLS = 8192


def draw_counts(key, part):
    first = jax.random.fold_in(key, 11)
    second = jax.random.fold_in(key, 12)
    third = jax.random.fold_in(key, 13)
    powers = jax.random.randint(first, (1, GENES), 0, 7)
    ceiling = jnp.left_shift(jnp.ones((1, GENES), jnp.int32), powers)
    values = jax.random.randint(second, (CELLS, GENES), 0, ceiling + 1)
    present = jax.random.randint(third, (CELLS, GENES), 0, 5) < 2
    return jnp.where(present, values, 0).astype(jnp.int32)


def draw_live_rows(key, part):
    first = jax.random.fold_in(key, 21)
    second = jax.random.fold_in(key, 22)
    lengths = jax.random.randint(first, (CELL_BLOCKS,), CELL_DEV // 2, CELL_DEV + 1)
    chosen = jax.random.randint(second, (), 0, CELL_BLOCKS)
    places = jnp.arange(CELL_BLOCKS, dtype=jnp.int32)
    return jnp.where(places == chosen, CELL_DEV, lengths).astype(jnp.int32)


def shard_levels(rng, shape, pieces, least, largest):
    def one(axis_at, parts):
        draws = jax.random.uniform(jax.random.fold_in(jax.random.fold_in(rng, 6), axis_at), (parts,), jnp.float32, least / len(pieces), largest / len(pieces))
        return jnp.repeat(jnp.exp(draws), shape[axis_at] // parts).reshape((-1,) + (1,) * (len(shape) - axis_at - 1))

    loudness = one(*pieces[0])
    for cut in pieces[1:]:
        loudness = loudness * one(*cut)
    return loudness


def centred(rng, shape, scale, reach, shards=(), kind=jnp.bfloat16):
    loudness = shard_levels(rng, shape, shards, -0.22, 0.18) if shards else 1.0
    drawn = jax.random.normal(rng, shape, jnp.float32) * scale * loudness
    return jnp.minimum(jnp.maximum(drawn, -reach), reach).astype(kind)


def setup_inputs(seed: int = 0) -> dict:
    keys = jax.random.split(jax.random.key(seed), 6)
    counts = draw_counts(jax.random.fold_in(keys[5], 71), 0)
    live_rows = draw_live_rows(jax.random.fold_in(keys[5], 71), 0)
    left_basis = centred(keys[2], (BASIS, CELLS), CELLS ** -0.5, 0.0625, ((1, 64),), jnp.float32)
    right_basis = centred(keys[3], (BASIS, GENES), GENES ** -0.5, 0.03125, ((1, 4),), jnp.float32)
    right_start = centred(keys[4], (BLOCK, GENES), GENES ** -0.5, 0.03125, ((1, 4),), jnp.float32)
    return {"counts": counts, "live_rows": live_rows, "left_basis": left_basis, "right_basis": right_basis, "right_start": right_start}


HIGHEST = lax.Precision.HIGHEST

def matmul(lhs, rhs):
    return jnp.dot(lhs.astype(jnp.float32), rhs.astype(jnp.float32), precision=HIGHEST, preferred_element_type=jnp.float32)

def outer_rows(lhs, rhs):
    return lax.dot_general(lhs.astype(jnp.float32), rhs.astype(jnp.float32), (((1,), (1,)), ((), ())), precision=HIGHEST, preferred_element_type=jnp.float32)

def orthonormal_block(vectors, spanning):
    coeffs = outer_rows(vectors, spanning)
    cleaned = vectors - matmul(coeffs, spanning)
    coeffs = outer_rows(cleaned, spanning)
    cleaned = cleaned - matmul(coeffs, spanning)
    squares = outer_rows(cleaned, cleaned)
    factor = jnp.linalg.cholesky(squares)
    result = lax.linalg.triangular_solve(factor, cleaned, left_side=True, lower=True)
    return (result, factor)

def reference(counts, live_rows, left_basis, right_basis, right_start):
    within = jnp.arange(CELL_DEV, dtype=jnp.int32)[None, :] < live_rows[:, None]
    weights = within.reshape(CELLS).astype(jnp.float32)
    logged = jnp.where(weights[:, None] > 0, jnp.log1p(counts.astype(jnp.float32)), 0.0)
    live_total = jnp.sum(live_rows).astype(jnp.float32)
    column_mean = lax.optimization_barrier(jnp.sum(logged, axis=0)) / live_total
    factor_scale = lax.rsqrt(live_total)
    slots_left = jnp.concatenate([left_basis * weights[None, :], jnp.zeros((STEPS * BLOCK, CELLS), jnp.float32)], axis=0)
    slots_right = jnp.concatenate([right_basis, right_start, jnp.zeros(((STEPS - 1) * BLOCK, GENES), jnp.float32)], axis=0)
    current = right_start
    left_blocks, right_blocks, diag_list, couple_list = ([], [], [], [])
    for iteration in range(STEPS):
        projected = (outer_rows(current, logged) - matmul(current, column_mean)[:, None] * weights[None, :]) * factor_scale
        leftvec, diag_factor = orthonormal_block(projected, slots_left)
        position = BASIS + iteration * BLOCK
        slots_left = slots_left.at[position:position + BLOCK].set(leftvec)
        projected = (matmul(leftvec, logged) - lax.optimization_barrier(jnp.sum(leftvec, axis=1))[:, None] * column_mean[None, :]) * factor_scale
        current, side_factor = orthonormal_block(projected, slots_right)
        if iteration + 1 < STEPS:
            slots_right = slots_right.at[position + BLOCK:position + 2 * BLOCK].set(current)
        left_blocks.append(leftvec)
        right_blocks.append(current)
        diag_list.append(diag_factor)
        couple_list.append(side_factor)
    left_vectors = jnp.concatenate(left_blocks, axis=0) * jnp.sqrt(jnp.float32(CELLS))
    right_vectors = jnp.concatenate(right_blocks, axis=0) * jnp.sqrt(jnp.float32(GENES))
    return (left_vectors, right_vectors, jnp.stack(diag_list), jnp.stack(couple_list))
```

```python
import math
import os

import jax
import jax.numpy as jnp
from jax import lax
from jax.experimental import pallas as pl
from jax.experimental.pallas import tpu as pltpu
from jax.sharding import Mesh
from jax.sharding import PartitionSpec as P

BASIS = 32
BLOCK = 16
STEPS = 3
ROWS = 128
TILE = 128
PIECES = 32
PEERS = 8
MAIN = PIECES * TILE
LOCAL = MAIN + TILE
HALF = TILE // 2
FAR = ("z", "y")
NEAR = ("core", "x")
F32 = jnp.float32
BF16 = jnp.bfloat16
PLAIN = False


def call(fn, name, outs, *args):
    if PLAIN:
        return fn(*args)
    count = len(args)

    def kernel(*refs):
        results = fn(*(r[...] for r in refs[:count]))
        for ref, value in zip(refs[count:], results):
            ref[...] = value

    return pl.pallas_call(
        kernel,
        out_shape=[jax.ShapeDtypeStruct(s, d) for s, d in outs],
        in_specs=[pl.BlockSpec(memory_space=pltpu.VMEM)] * count,
        out_specs=[pl.BlockSpec(memory_space=pltpu.VMEM)] * len(outs),
        compiler_params=pltpu.CompilerParams(vmem_limit_bytes=48 * 1024 * 1024),
        name=name,
    )(*args)


def roll(value, shift, axis):
    size = value.shape[axis]
    return jnp.roll(value, shift, axis) if PLAIN else pltpu.roll(value, shift % size, axis)


def mm(lhs, rhs):
    return lax.dot_general(lhs, rhs, (((1,), (0,)), ((), ())), precision=lax.Precision.HIGHEST, preferred_element_type=F32)


def mt(lhs, rhs):
    return lax.dot_general(lhs, rhs, (((1,), (1,)), ((), ())), precision=lax.Precision.HIGHEST, preferred_element_type=F32)


def tm(lhs, rhs):
    return lax.dot_general(lhs, rhs, (((0,), (0,)), ((), ())), precision=lax.Precision.HIGHEST, preferred_element_type=F32)


def two(value):
    high = value.astype(BF16)
    return jnp.concatenate([high, (value - high.astype(F32)).astype(BF16)], axis=0)


def folded(value):
    half = value.shape[0] // 2
    return value[:half] + value[half:]


def fine_mt(pair, high, low):
    dims = (((1,), (1,)), ((), ()))
    return folded(
        lax.dot_general(pair, high, dims, preferred_element_type=F32)
        + lax.dot_general(pair, low, dims, preferred_element_type=F32)
    )


def fine_mm(pair, high, low):
    dims = (((1,), (0,)), ((), ()))
    return folded(
        lax.dot_general(pair, high, dims, preferred_element_type=F32)
        + lax.dot_general(pair, low, dims, preferred_element_type=F32)
    )


def zeros(rows, lanes=TILE, dtype=F32):
    return jnp.zeros((rows, lanes), dtype)


def at_rows(value, start, rows=TILE):
    count, lanes = value.shape
    parts = []
    if start:
        parts.append(zeros(start, lanes, value.dtype))
    parts.append(value)
    if start + count < rows:
        parts.append(zeros(rows - start - count, lanes, value.dtype))
    return jnp.concatenate(parts, axis=0)


def lanes_of(shape):
    return lax.broadcasted_iota(jnp.int32, shape, 1)


def rows_of(shape):
    return lax.broadcasted_iota(jnp.int32, shape, 0)


def lane_range(value, start, stop):
    lane = lanes_of(value.shape)
    return jnp.where((lane >= start) & (lane < stop), value, 0.0)


def widened(value):
    return jnp.concatenate([value, zeros(value.shape[0], TILE - value.shape[1])], axis=1)


def factored(squares):
    lane = lanes_of((BLOCK, TILE))
    row = rows_of((BLOCK, TILE))
    work = squares + jnp.where(lane == row + BLOCK, 1.0, 0.0)
    factor = jnp.zeros((BLOCK, TILE), F32)
    for k in range(BLOCK):
        column = jnp.broadcast_to(work[:, k : k + 1], (BLOCK, TILE))
        scale = 1.0 / jnp.sqrt(jnp.broadcast_to(column[k : k + 1], (BLOCK, TILE)))
        column = column * scale
        pivot = work[k : k + 1] * scale
        factor = jnp.where((lane == k) & (row >= k), column, factor)
        work = jnp.where(row > k, work - column * pivot, jnp.where(row == k, pivot, work))
    return factor, lane_range(work, BLOCK, 2 * BLOCK)


def orthonormal(coeffs, squares, correlations, position):
    against = mm(coeffs, correlations)
    combined = coeffs + coeffs - against
    passed = mm(combined, correlations)
    remaining = squares + widened(mt(passed - coeffs, combined) - mt(combined, coeffs))
    factor, shifted = factored(remaining)
    inverse = lane_range(roll(shifted, -BLOCK, 1), 0, BLOCK)
    residual = mm(inverse[:, :BLOCK], coeffs - passed)
    identity = jnp.where(lanes_of((BLOCK, TILE)) == rows_of((BLOCK, TILE)) + position, 1.0, 0.0)
    full = residual + identity
    if position + BLOCK <= TILE:
        placed = at_rows(residual, position)
        correlations = correlations + placed + placed.T + at_rows(identity, position)
    return combined, factor, inverse, full, correlations


def tiles(value, start, rows):
    return [value[start : start + rows, p * TILE : (p + 1) * TILE] for p in range(PIECES)]


def near_message(parts, core):
    own, other = parts[0]
    blocks = []
    for target in range(2):
        same = core[0, 0] == target
        rows = []
        for a, b in parts:
            if b is None:
                rows.append(a)
            else:
                rows += [jnp.where(same, a, b), jnp.where(same, b, a)]
        block = jnp.concatenate(rows, axis=0)
        blocks += [block] * (PEERS // 2)
    return jnp.stack(blocks)


def halves(value):
    return value[:, :TILE], value[:, TILE:]


def start_kernel(core, high, low, basis, block):
    lead = two(jnp.concatenate([basis, block], axis=0))
    image = fine_mt(lead, high, low)
    count = BASIS + BLOCK
    gram = fine_mt(lead, jnp.concatenate([lead[:count], jnp.zeros((TILE - count, LOCAL), BF16)], axis=0),
                   jnp.concatenate([lead[count:], jnp.zeros((TILE - count, LOCAL), BF16)], axis=0))
    message = near_message([halves(image), (gram, None)], core)
    return message, lead


def first_cells(arrived, weights, left_basis, high, low):
    total = jnp.sum(arrived, axis=0)
    count = BASIS + BLOCK
    image = jnp.concatenate([total[:count], total[count : 2 * count]], axis=1)
    correlations = at_rows(total[2 * count :], 0)
    weight = weights[:1]
    basis_image, block_image = image[:BASIS], image[BASIS:]
    weighted = left_basis * weight
    ones = jnp.broadcast_to(weight, (8, weight.shape[1]))
    stack = jnp.concatenate([weighted, block_image, basis_image, ones, zeros(TILE - 88, 2 * TILE)], axis=0)
    sums = mt(ones, stack)
    live = jnp.sum(weight, axis=1, keepdims=True)
    centred_basis = weighted - jnp.sum(weighted, axis=1, keepdims=True) / live * weight
    centred_block = block_image - jnp.sum(block_image, axis=1, keepdims=True) / live * weight
    lead = jnp.concatenate([centred_basis, centred_block, ones, zeros(8, 2 * TILE)], axis=0)
    product = fine_mm(two(lead), high, low)
    spare = jnp.concatenate([product[:, MAIN:], zeros(TILE - 64)], axis=0).T
    grams = mt(centred_block, jnp.concatenate([weighted, centred_block, zeros(80, 2 * TILE)], axis=0))
    grams += mt(weighted[:BLOCK], jnp.concatenate([zeros(64, 2 * TILE), weighted, zeros(32, 2 * TILE)], axis=0))
    grams += mt(weighted[BLOCK:], jnp.concatenate([zeros(96, 2 * TILE), weighted], axis=0))
    row = rows_of((8, TILE))
    pieces = []
    for p in range(PIECES):
        main = product[:56, p * TILE : (p + 1) * TILE]
        tail = jnp.where(row == 0, main[48:], 0.0)
        tail = jnp.where(row == 1, spare[p : p + 1], tail)
        tail = jnp.where(row == 2, spare[PIECES + p : PIECES + p + 1], tail)
        tail = jnp.where(row == 3, sums, tail)
        pieces.append(jnp.concatenate([main[:48], tail, grams], axis=0))
    return jnp.stack(pieces), image, correlations, weighted


def copies(block):
    return jnp.broadcast_to(block[None], (PIECES, *block.shape))


def solved_piece(main, spare, combined, inverse, slots, spare_slots, position):
    inner = inverse[:, :BLOCK]
    piece = mm(inner, main - mm(combined, slots))
    rows = mt(spare[:, :BLOCK] - mt(spare_slots, combined), inner)
    slots = slots + at_rows(piece, position)
    rows = widened(rows)
    spare_slots = spare_slots + roll(rows, position, 1)
    return piece, rows, slots, spare_slots


def first_piece(arrived):
    total = jnp.sum(arrived, axis=0)
    sums = arrived[:, 51, :]
    every = total[51:52]
    lane = lanes_of(sums.shape)
    live = jnp.broadcast_to(sums[:, 80:81], sums.shape)
    whole = jnp.broadcast_to(every[:, 80:81], every.shape)
    scale = lax.rsqrt(whole)
    means = sums / live
    block_lane = (lane >= BASIS) & (lane < BASIS + BLOCK)
    weights = jnp.where(block_lane, means - every / whole, jnp.where(lane < BASIS, means, 0.0))
    column_mean = total[48:49] / whole
    spread = arrived[:, 48, :] - live * column_mean
    main = total[:48] + tm(weights, spread)[:48]
    spare = []
    spare_mean = []
    for k in range(2):
        mean = jnp.broadcast_to(total[49 + k : 50 + k, 48:49], (1, TILE)) / whole
        column = jnp.broadcast_to(arrived[:, 49 + k, 48:49], sums.shape) - live * mean
        spare.append(total[49 + k : 50 + k] + jnp.sum(weights * column, axis=0, keepdims=True))
        spare_mean.append(mean)
    gram = total[56:72]
    between = tm(weights, jnp.where(lane < BASIS, sums, live * weights))[BASIS : BASIS + BLOCK]
    inner = gram + between
    scale16 = jnp.broadcast_to(scale, (BLOCK, TILE))
    coeffs = lane_range(inner, 0, BASIS) * scale16
    squares = lane_range(roll(inner, -BASIS, 1), 0, BLOCK) * scale16 * scale16
    low = roll(gram, -64, 1)
    basis_gram = jnp.concatenate([lane_range(low, 0, BASIS), lane_range(roll(gram, -96, 1), 0, BASIS)], axis=0)
    correlations = at_rows(basis_gram, 0)
    combined, factor, inverse, full, correlations = orthonormal(coeffs, squares, correlations, BASIS)
    row8 = rows_of((8, TILE))
    both = jnp.where(row8 == 0, spare[0], jnp.where(row8 == 1, spare[1], 0.0)) * scale
    slots = at_rows(main[:BASIS] * jnp.broadcast_to(scale, (BASIS, TILE)), 0)
    spare_slots = lane_range(both, 0, BASIS)
    block_main = main[BASIS:] * scale16 * scale16
    block_spare = lane_range(roll(both, -BASIS, 1), 0, BLOCK) * scale
    piece, rows, slots, spare_slots = solved_piece(block_main, block_spare, combined, inverse, slots, spare_slots, BASIS)
    lane8 = lanes_of((8, TILE))
    marks = jnp.where(row8 == 0, spare_mean[0], spare_mean[1])
    tail = jnp.where(row8 < 2, jnp.where(lane8 == BLOCK, marks, rows), jnp.where(row8 == 2, column_mean, 0.0))
    means8 = jnp.where(row8 == 0, column_mean, jnp.where(row8 == 1, spare_mean[0], jnp.where(row8 == 2, spare_mean[1], 0.0)))
    stats = jnp.where(row8 == 0, scale, jnp.where(row8 == 1, every / whole, 0.0))
    message = copies(jnp.concatenate([piece, tail], axis=0))
    return message, combined, factor, inverse, correlations, slots, spare_slots, means8, stats


def later_piece(position):
    def fn(arrived, known, correlations, slots, spare_slots, means8, stats):
        total = jnp.sum(arrived, axis=0)
        tile = total[BLOCK:]
        gram = jnp.concatenate([tile, roll(tile, -HALF, 1)], axis=0)
        coeffs = lane_range(gram, 0, BASIS) + known
        squares = lane_range(roll(gram, -BASIS, 1), 0, BLOCK)
        combined, factor, inverse, full, correlations = orthonormal(coeffs, squares, correlations, position)
        scale = stats[:1]
        rows = lane_range(roll(tile, -48, 1), 0, BLOCK)
        row8 = rows_of((8, TILE))
        sums = jnp.broadcast_to(rows[2:3], (8, TILE))
        outer = tm(jnp.where(row8 == 0, sums, 0.0), jnp.where(row8 == 0, jnp.broadcast_to(means8[:1], (8, TILE)), 0.0))[:BLOCK]
        main = (total[:BLOCK] - outer) * jnp.broadcast_to(scale, (BLOCK, TILE))
        spare_mean = jnp.where(row8 == 0, means8[1:2], jnp.where(row8 == 1, means8[2:3], 0.0))
        spare = jnp.where(row8 < 2, (rows - sums * spare_mean) * scale, 0.0)
        piece, fresh, slots, spare_slots = solved_piece(main, spare, combined, inverse, slots, spare_slots, position)
        message = copies(jnp.concatenate([piece, jnp.where(row8 < 2, fresh, 0.0)], axis=0))
        return message, combined, factor, inverse, correlations, slots, spare_slots
    return fn


def gathered(arrived):
    spare = jnp.concatenate([arrived[:, 16, :], arrived[:, 17, :], zeros(TILE - 2 * PIECES)], axis=0).T
    block = jnp.concatenate([arrived[p, :BLOCK] for p in range(PIECES)] + [lane_range(spare[:BLOCK], 0, HALF)], axis=1)
    return block, spare


def gene_sums(block, mean, core, weights, high, low, bases):
    pair = two(block)
    image = fine_mt(pair, high, low)
    mean_pair = two(jnp.broadcast_to(mean, (BLOCK, LOCAL)))
    known = sum(b.shape[0] // 2 for b in bases)
    gap = jnp.zeros((80 - known, LOCAL), BF16)
    end = jnp.zeros((BLOCK, LOCAL), BF16)
    tops = [b[: b.shape[0] // 2] for b in bases] + ([gap] if known < 80 else []) + [pair[:BLOCK], mean_pair[:BLOCK], end]
    lows = [b[b.shape[0] // 2 :] for b in bases] + ([gap] if known < 80 else []) + [pair[BLOCK:], mean_pair[BLOCK:], end]
    gram = fine_mt(pair, jnp.concatenate(tops, axis=0), jnp.concatenate(lows, axis=0))
    image = image - gram[:, 96:97] * weights[:1]
    return near_message([halves(image), (lane_range(gram, 0, 96), None)], core)


def first_genes(arrived, core, weights, high, low, *bases):
    block, spare = gathered(arrived)
    mean = jnp.concatenate([arrived[p, 18:19] for p in range(PIECES)] + [lane_range(spare[BLOCK : BLOCK + 1], 0, HALF)], axis=1)
    return gene_sums(block, mean, core, weights, high, low, bases), block, mean


def later_genes(arrived, mean, core, weights, high, low, *bases):
    block, _ = gathered(arrived)
    return gene_sums(block, mean, core, weights, high, low, bases), block


def right_orth(arrived, correlations, position):
    total = jnp.sum(arrived, axis=0)
    image = jnp.concatenate([total[:BLOCK], total[BLOCK : 2 * BLOCK]], axis=1)
    gram = total[2 * BLOCK :]
    coeffs = lane_range(gram, 0, 80)
    squares = lane_range(roll(gram, -80, 1), 0, BLOCK)
    return (image,) + orthonormal(coeffs, squares, correlations, position)


def later_cells(step):
    position = BASIS + step * BLOCK

    def fn(arrived, correlations, images, expansions, weights, weighted, stats, high, low):
        image, combined, factor, inverse, full, correlations = right_orth(arrived, correlations, position)
        scale = stats[:1, :1]
        block = mm(inverse[:, :BLOCK], image * scale - mm(combined, images))
        images = images + at_rows(block, position)
        expansions = expansions + at_rows(combined + roll(factor, position, 1), position - BLOCK)
        known = mt(full, expansions)
        product = fine_mm(two(block), high, low)
        gram = mt(block, jnp.concatenate([weighted, block, zeros(80, 2 * TILE)], axis=0))
        sums = mt(jnp.broadcast_to(weights[:1], (8, 2 * TILE)), at_rows(block, 48))
        spare = at_rows(product[:, MAIN:], 48).T
        row8 = rows_of((8, TILE))
        tile = gram[:8] + roll(gram[8:], HALF, 1) + jnp.where(row8 == 2, sums, 0.0)
        pieces = []
        for p in range(PIECES):
            tail = tile + jnp.where(row8 == 0, spare[p : p + 1], jnp.where(row8 == 1, spare[PIECES + p : PIECES + p + 1], 0.0))
            pieces.append(jnp.concatenate([product[:, p * TILE : (p + 1) * TILE], tail], axis=0))
        return jnp.stack(pieces), combined, factor, inverse, known, correlations, images, expansions, block
    return fn


def last_cells(arrived, correlations):
    image, combined, factor, inverse, full, correlations = right_orth(arrived, correlations, BASIS + STEPS * BLOCK)
    return combined, factor, inverse


def first_images(image, stats, weights):
    scale = stats[:1, :1]
    both = image
    means = stats[1:2]
    means = jnp.concatenate([means[:, 48:80], means[:, BASIS : BASIS + BLOCK]], axis=1)
    column = jnp.broadcast_to(means, (8, 48)).T[:, :1] if PLAIN else widened(jnp.broadcast_to(means, (8, 48)))
    if not PLAIN:
        column = at_rows(column, 0).T[:48, :1]
    return (at_rows((both - column * weights[:1]) * scale, 0),)


def new_right(block, combined, inverse, *bases):
    known = sum(b.shape[0] // 2 for b in bases)
    high = jnp.concatenate([b[: b.shape[0] // 2] for b in bases], axis=0)
    low = jnp.concatenate([b[b.shape[0] // 2 :] for b in bases], axis=0)
    cleaned = block - fine_mm(two(combined[:, :known]), high, low)
    value = mm(inverse[:, :BLOCK], cleaned)
    return value, two(value)


def new_left(block, combined, inverse, slots, position):
    value = mm(inverse[:, :BLOCK], block - mm(combined, slots))
    return value, slots + at_rows(value, position)


def far(value):
    return lax.all_to_all(value, FAR, split_axis=0, concat_axis=0, tiled=True)


def near(value):
    return lax.all_to_all(value, NEAR, split_axis=0, concat_axis=0, tiled=True)


def partner(value):
    return lax.ppermute(value, "core", [(0, 1), (1, 0)])


def own_genes(value, core):
    main = lax.dynamic_slice_in_dim(value, core * MAIN, MAIN, 1)
    spare = jnp.where(core == 0, value[:, 2 * MAIN : 2 * MAIN + HALF], value[:, 2 * MAIN + HALF :])
    return jnp.concatenate([main, jnp.pad(spare, ((0, 0), (0, HALF)))], axis=1)


def all_genes(own, other, core):
    first = jnp.where(core == 0, own, other)
    second = jnp.where(core == 0, other, own)
    return jnp.concatenate([first[:, :MAIN], second[:, :MAIN], first[:, MAIN : MAIN + HALF], second[:, MAIN : MAIN + HALF]], axis=1)


def body(counts, live_rows, left_basis, right_basis, right_start):
    core = lax.axis_index("core")
    core_index = jnp.full((1, 1), core, jnp.int32)
    live = live_rows[0]
    sent = own_genes(counts, 1 - core)
    got = partner(sent)
    cells = jnp.arange(ROWS, dtype=jnp.int32)
    weight = (cells < live).astype(F32)
    bundle = jnp.concatenate([left_basis, jnp.broadcast_to(weight, (8, ROWS))], axis=0)
    got_bundle = partner(bundle)
    weights = jnp.concatenate([bundle[BASIS:], got_bundle[BASIS:]], axis=1)
    basis_left = jnp.concatenate([left_basis, got_bundle[:BASIS]], axis=1)
    every = jnp.concatenate([own_genes(counts, core), got], axis=0)
    logged = jnp.where(weights[0][:, None] > 0, jnp.log1p(every.astype(F32)), 0.0)
    top = lax.reduce_precision(logged, 8, 7)
    high, low = top.astype(BF16), (logged - top).astype(BF16)
    basis_right = own_genes(right_basis, core)
    start = own_genes(right_start, core)

    square = ((TILE, TILE), F32)
    slim = ((BLOCK, TILE), F32)
    small = ((8, TILE), F32)
    wide = ((BLOCK, 2 * TILE), F32)
    tall = ((TILE, 2 * TILE), F32)
    long = ((BLOCK, LOCAL), F32)
    row = ((1, LOCAL), F32)
    count = BASIS + BLOCK

    message, lead = call(start_kernel, "start", [((PEERS, 3 * count, TILE), F32), ((2 * count, LOCAL), BF16)],
                         core_index, high, low, basis_right, start)
    bases = [lead]
    arrived = near(message)
    message, image, right_corr, weighted = call(
        first_cells, "first_cells",
        [((PIECES, 72, TILE), F32), ((count, 2 * TILE), F32), square, ((BASIS, 2 * TILE), F32)],
        arrived, weights, basis_left, high, low)
    arrived = far(message)
    lefts, rights, diags, couples = [], [], [], []
    left_slots = jnp.pad(weighted, ((0, TILE - BASIS), (0, 0)))
    expansions = jnp.zeros((TILE, TILE), F32)
    for step in range(STEPS):
        position = BASIS + step * BLOCK
        if step == 0:
            message, combined, factor, inverse, left_corr, slots, spare_slots, means8, stats = call(
                first_piece, "first_piece",
                [((PIECES, 24, TILE), F32), slim, slim, slim, square, square, small, small, small], arrived)
        else:
            message, combined, factor, inverse, left_corr, slots, spare_slots = call(
                later_piece(position), "piece",
                [((PIECES, 24, TILE), F32), slim, slim, slim, square, square, small],
                arrived, known, left_corr, slots, spare_slots, means8, stats)
        arrived = far(message)
        diags.append(factor[:, :BLOCK])
        if step == 0:
            (images,) = call(first_images, "first_images", [tall], image, stats, weights)
            block = images[BASIS : BASIS + BLOCK]
        left, left_slots = call(
            lambda a, b, c, d, position=position: new_left(a, b, c, d, position), "new_left", [wide, tall],
            block, combined, inverse, left_slots)
        lefts.append(left[:, :ROWS])
        message_shape = ((PEERS, 3 * BLOCK, TILE), F32)
        if step == 0:
            message, genes_block, mean = call(first_genes, "first_genes", [message_shape, long, row],
                                              arrived, core_index, weights, high, low, *bases)
        else:
            message, genes_block = call(later_genes, "genes", [message_shape, long],
                                        arrived, mean, core_index, weights, high, low, *bases)
        arrived = near(message)
        if step + 1 < STEPS:
            message, combined, factor, inverse, known, right_corr, images, expansions, block = call(
                later_cells(step + 1), "cells",
                [((PIECES, 24, TILE), F32), slim, slim, slim, slim, square, tall, square, wide],
                arrived, right_corr, images, expansions, weights, weighted, stats, high, low)
            arrived = far(message)
        else:
            combined, factor, inverse = call(last_cells, "last_cells", [slim, slim, slim], arrived, right_corr)
        couples.append(factor[:, :BLOCK])
        value, pair = call(new_right, "new_right", [long, ((2 * BLOCK, LOCAL), BF16)],
                           genes_block, combined, inverse, *bases)
        bases = bases + [pair]
        rights.append(all_genes(value, partner(value), core))
    left_vectors = jnp.concatenate(lefts, axis=0) * math.sqrt(8192.0)
    right_vectors = jnp.concatenate(rights, axis=0) * math.sqrt(33280.0)
    return left_vectors, right_vectors, jnp.stack(diags), jnp.stack(couples)


def solution(mesh):
    split = Mesh(mesh.devices.reshape(8, 4, 2, 4), ("z", "y", "core", "x"))
    cells = ("z", "y", "core")
    return jax.shard_map(
        body,
        mesh=split,
        in_specs=(P(cells, "x"), P(cells), P(None, cells), P(None, "x"), P(None, "x")),
        out_specs=(P(None, cells), P(None, "x"), P(), P()),
        check_vma=False,
    )
```

```python
import math
import os

import jax
import jax.numpy as jnp
from jax import lax
from jax.experimental import pallas as pl
from jax.experimental.pallas import tpu as pltpu
from jax.sharding import Mesh
from jax.sharding import PartitionSpec as P

BASIS = 32
BLOCK = 16
STEPS = 3
ROWS = 128
TILE = 128
PIECES = 32
PEERS = 8
MAIN = PIECES * TILE
LOCAL = MAIN + TILE
CHUNKS = 3
SMALL = 40000
CHUNK = LOCAL // CHUNKS
HALF = TILE // 2
FAR = ("z", "y")
NEAR = ("core", "x")
F32 = jnp.float32
BF16 = jnp.bfloat16


def in_hbm(value):
    return pltpu.with_memory_space_constraint(value, pltpu.HBM)


def is_small(shape):
    return math.prod(shape) <= SMALL


def call(fn, name, outs, *args, streams=(), arrived=False):
    held = [is_small(a.shape) or n < int(arrived) for n, a in enumerate(args)]
    args = [a if h else in_hbm(a) for a, h in zip(args, held)]
    whole = list(streams[:1])
    streams = [in_hbm(a) for a in streams[1:]]
    count, kept, given = len(args), len(streams), len(outs)
    first = len(whole)
    loaded = [n for n in range(count) if not held[n]]
    stored = [n for n in range(given) if not is_small(outs[n][0])]
    total = len(loaded) + len(stored) + kept * CHUNKS

    def kernel(*refs):
        operands = refs[:count]
        resident = refs[count : count + first]
        sources = refs[count + first : count + first + kept]
        results = refs[count + first + kept : count + first + kept + given]
        scratch = refs[count + first + kept + given :]
        inside = scratch[: len(loaded)]
        written = scratch[len(loaded) : len(loaded) + len(stored)]
        parts = scratch[len(loaded) + len(stored) : len(loaded) + len(stored) + kept]
        semaphores = scratch[-1] if total else None
        entering = [pltpu.make_async_copy(operands[n], inside[m], semaphores.at[m]) for m, n in enumerate(loaded)]
        base = len(loaded) + len(stored)
        streaming = []
        for k in range(CHUNKS):
            window = (slice(None), pl.ds(k * CHUNK, CHUNK))
            streaming.append([
                pltpu.make_async_copy(source.at[window], parts[n].at[window], semaphores.at[base + n * CHUNKS + k])
                for n, source in enumerate(sources)
            ])
        for copy in entering:
            copy.start()
        for group in streaming:
            for copy in group:
                copy.start()

        def chunk(k):
            for copy in streaming[k]:
                copy.wait()
            return [ref[:, k * CHUNK : (k + 1) * CHUNK] for ref in (*resident, *parts)]

        for copy in entering:
            copy.wait()
        values = [operands[n][...] if held[n] else inside[loaded.index(n)][...] for n in range(count)]
        leaving = []
        for n, value in enumerate(fn(*values, chunk) if kept else fn(*values)):
            if n not in stored:
                results[n][...] = value
                continue
            place = written[stored.index(n)]
            place[...] = value
            copy = pltpu.make_async_copy(place, results[n], semaphores.at[len(loaded) + stored.index(n)])
            copy.start()
            leaving.append(copy)
        for copy in leaving:
            copy.wait()

    vmem = pl.BlockSpec(memory_space=pltpu.VMEM)
    hbm = pl.BlockSpec(memory_space=pltpu.HBM)
    scratch_shapes = [pltpu.VMEM(args[n].shape, args[n].dtype) for n in loaded]
    scratch_shapes += [pltpu.VMEM(*outs[n]) for n in stored]
    scratch_shapes += [pltpu.VMEM(a.shape, a.dtype) for a in streams]
    if total:
        scratch_shapes.append(pltpu.SemaphoreType.DMA((total,)))
    return pl.pallas_call(
        kernel,
        out_shape=[pltpu.HBM(s, d) if n in stored else jax.ShapeDtypeStruct(s, d) for n, (s, d) in enumerate(outs)],
        in_specs=[vmem if h else hbm for h in held] + [vmem] * first + [hbm] * kept,
        out_specs=[hbm if n in stored else vmem for n in range(given)],
        scratch_shapes=scratch_shapes,
        compiler_params=pltpu.CompilerParams(vmem_limit_bytes=32 * 1024 * 1024),
        name=name,
    )(*args, *whole, *streams)


def roll(value, shift, axis):
    size = value.shape[axis]
    return pltpu.roll(value, shift % size, axis)


def mm(lhs, rhs):
    return lax.dot_general(lhs, rhs, (((1,), (0,)), ((), ())), precision=lax.Precision.HIGHEST, preferred_element_type=F32)


def mt(lhs, rhs):
    return lax.dot_general(lhs, rhs, (((1,), (1,)), ((), ())), precision=lax.Precision.HIGHEST, preferred_element_type=F32)


def tm(lhs, rhs):
    return lax.dot_general(lhs, rhs, (((0,), (0,)), ((), ())), precision=lax.Precision.HIGHEST, preferred_element_type=F32)


def two(value):
    high = value.astype(BF16)
    return jnp.concatenate([high, (value - high.astype(F32)).astype(BF16)], axis=0)


def folded(value):
    half = value.shape[0] // 2
    return value[:half] + value[half:]


def fine_mt(pair, high, low):
    dims = (((1,), (1,)), ((), ()))
    return folded(
        lax.dot_general(pair, high, dims, preferred_element_type=F32)
        + lax.dot_general(pair, low, dims, preferred_element_type=F32)
    )


def fine_mm(pair, high, low):
    dims = (((1,), (0,)), ((), ()))
    return folded(
        lax.dot_general(pair, high, dims, preferred_element_type=F32)
        + lax.dot_general(pair, low, dims, preferred_element_type=F32)
    )


def stream_mt(pair, chunk):
    dims = (((1,), (1,)), ((), ()))
    total = None
    for k in range(CHUNKS):
        part = pair[:, k * CHUNK : (k + 1) * CHUNK]
        for matrix in chunk(k):
            one = lax.dot_general(part, matrix, dims, preferred_element_type=F32)
            total = one if total is None else total + one
    return folded(total)


def stream_mm(pair, chunk):
    dims = (((1,), (0,)), ((), ()))
    parts = []
    for k in range(CHUNKS):
        high, low = chunk(k)
        parts.append(
            folded(
                lax.dot_general(pair, high, dims, preferred_element_type=F32)
                + lax.dot_general(pair, low, dims, preferred_element_type=F32)
            )
        )
    return jnp.concatenate(parts, axis=1)


def zeros(rows, lanes=TILE, dtype=F32):
    return jnp.zeros((rows, lanes), dtype)


def at_rows(value, start, rows=TILE):
    count, lanes = value.shape
    parts = []
    if start:
        parts.append(zeros(start, lanes, value.dtype))
    parts.append(value)
    if start + count < rows:
        parts.append(zeros(rows - start - count, lanes, value.dtype))
    return jnp.concatenate(parts, axis=0)


def lanes_of(shape):
    return lax.broadcasted_iota(jnp.int32, shape, 1)


def rows_of(shape):
    return lax.broadcasted_iota(jnp.int32, shape, 0)


def lane_range(value, start, stop):
    lane = lanes_of(value.shape)
    return jnp.where((lane >= start) & (lane < stop), value, 0.0)


def widened(value):
    return jnp.concatenate([value, zeros(value.shape[0], TILE - value.shape[1])], axis=1)


def factored(squares):
    lane = lanes_of((BLOCK, TILE))
    row = rows_of((BLOCK, TILE))
    work = squares + jnp.where(lane == row + BLOCK, 1.0, 0.0)
    factor = jnp.zeros((BLOCK, TILE), F32)
    for k in range(BLOCK):
        column = jnp.broadcast_to(work[:, k : k + 1], (BLOCK, TILE))
        scale = 1.0 / jnp.sqrt(jnp.broadcast_to(column[k : k + 1], (BLOCK, TILE)))
        column = column * scale
        pivot = work[k : k + 1] * scale
        factor = jnp.where((lane == k) & (row >= k), column, factor)
        work = jnp.where(row > k, work - column * pivot, jnp.where(row == k, pivot, work))
    return factor, lane_range(work, BLOCK, 2 * BLOCK)


def combination(coeffs, correlations):
    return coeffs + coeffs - mm(coeffs, correlations)


def scaled(raw, inverse):
    inner = inverse[:, :BLOCK]
    return widened(mt(mm(inner, raw[:, :BLOCK]), inner))


def orthonormal(coeffs, combined, squares, correlations, position):
    passed = mm(combined, correlations)
    remaining = squares + widened(mt(passed - coeffs, combined) - mt(combined, coeffs))
    factor, shifted = factored(remaining)
    inverse = lane_range(roll(shifted, -BLOCK, 1), 0, BLOCK)
    residual = mm(inverse[:, :BLOCK], coeffs - passed)
    identity = jnp.where(lanes_of((BLOCK, TILE)) == rows_of((BLOCK, TILE)) + position, 1.0, 0.0)
    full = residual + identity
    if position + BLOCK <= TILE:
        placed = at_rows(residual, position)
        correlations = correlations + placed + placed.T + at_rows(identity, position)
    return factor, inverse, full, correlations


def tiles(value, start, rows):
    return [value[start : start + rows, p * TILE : (p + 1) * TILE] for p in range(PIECES)]


def near_blocks(parts, core):
    blocks = []
    for target in range(2):
        same = core[0, 0] == target
        rows = []
        for a, b in parts:
            if b is None:
                rows.append(a)
            else:
                rows += [jnp.where(same, a, b), jnp.where(same, b, a)]
        blocks.append(jnp.concatenate(rows, axis=0))
    return blocks


def near_message(parts, core):
    blocks = near_blocks(parts, core)
    return jnp.stack([blocks[n // (PEERS // 2)] for n in range(PEERS)])


def halves(value):
    return value[:, :TILE], value[:, TILE:]


def start_kernel(basis, block, chunk):
    lead = two(jnp.concatenate([basis, block], axis=0))
    image = stream_mt(lead, chunk)
    count = BASIS + BLOCK
    gram = fine_mt(lead, jnp.concatenate([lead[:count], jnp.zeros((TILE - count, LOCAL), BF16)], axis=0),
                   jnp.concatenate([lead[count:], jnp.zeros((TILE - count, LOCAL), BF16)], axis=0))
    own, other = halves(image)
    return jnp.concatenate([own, other, gram], axis=0), jnp.concatenate([other, own, gram], axis=0), lead


def basis_cells(weights, left_basis, chunk):
    weight = weights[:1]
    weighted = left_basis * weight
    ones = jnp.broadcast_to(weight, (8, weight.shape[1]))
    sums = mt(ones, jnp.concatenate([weighted, zeros(48, 2 * TILE), ones, zeros(TILE - 88, 2 * TILE)], axis=0))
    live = jnp.sum(weight, axis=1, keepdims=True)
    centred = weighted - jnp.sum(weighted, axis=1, keepdims=True) / live * weight
    lead = jnp.concatenate([centred, zeros(BLOCK, 2 * TILE), ones, zeros(8, 2 * TILE)], axis=0)
    product = stream_mm(two(lead), chunk)
    spare = jnp.concatenate([product[:, MAIN:], zeros(TILE - 64)], axis=0).T
    gram = mt(weighted, at_rows(weighted, 0))
    folds = gram[:8]
    for n in range(1, 4):
        folds = folds + roll(gram[8 * n : 8 * n + 8], BASIS * n, 1)
    row = rows_of((8, TILE))
    pieces = []
    for p in range(PIECES):
        main = product[:, p * TILE : (p + 1) * TILE]
        tail = jnp.where(row == 0, main[48:56], 0.0)
        tail = jnp.where(row == 1, spare[p : p + 1], tail)
        tail = jnp.where(row == 2, spare[PIECES + p : PIECES + p + 1], tail)
        tail = jnp.where(row == 3, sums, tail)
        pieces.append(jnp.concatenate([main[:BASIS], tail, folds], axis=0))
    return jnp.stack(pieces), weighted


def block_message(product, gram, rows):
    spare = at_rows(product[:, MAIN:], 48).T
    row8 = rows_of((8, TILE))
    tile = gram[:8] + roll(gram[8:], HALF, 1) + rows
    pieces = []
    for p in range(PIECES):
        tail = tile + jnp.where(row8 == 0, spare[p : p + 1], jnp.where(row8 == 1, spare[PIECES + p : PIECES + p + 1], 0.0))
        pieces.append(jnp.concatenate([product[:, p * TILE : (p + 1) * TILE], tail], axis=0))
    return jnp.stack(pieces)


def first_cells(arrived, weights, weighted, chunk):
    total = jnp.sum(arrived, axis=0)
    count = BASIS + BLOCK
    image = jnp.concatenate([total[:count], total[count : 2 * count]], axis=1)
    correlations = at_rows(total[2 * count :], 0)
    weight = weights[:1]
    block = image[BASIS:]
    ones = jnp.broadcast_to(weight, (8, weight.shape[1]))
    row8 = rows_of((8, TILE))
    rows = jnp.where(row8 == 2, mt(ones, at_rows(block, 48)), 0.0)
    for n in range(2):
        rows = rows + jnp.where(row8 == 3 + n, mt(ones, at_rows(image[BLOCK * n : BLOCK * n + BLOCK], 48)), 0.0)
    live = jnp.sum(weight, axis=1, keepdims=True)
    centred = block - jnp.sum(block, axis=1, keepdims=True) / live * weight
    gram = mt(centred, jnp.concatenate([weighted, centred, zeros(80, 2 * TILE)], axis=0))
    return block_message(stream_mm(two(centred), chunk), gram, rows), image, correlations


def copies(block):
    return jnp.broadcast_to(block[None], (PIECES, *block.shape))


def cleaned_piece(main, spare, combined, slots, spare_slots):
    return main - mm(combined, slots), widened(spare[:, :BLOCK] - mt(spare_slots, combined))


def piece_state(position):
    def fn(raw, before, coeffs, combined, correlations, slots, spare_slots, piece, rows):
        squares = scaled(raw, before)
        factor, inverse, _, correlations = orthonormal(coeffs, combined, squares, correlations, position)
        inner = inverse[:, :BLOCK]
        slots = slots + at_rows(mm(inner, piece), position)
        spare_slots = spare_slots + roll(widened(mt(rows[:, :BLOCK], inner)), position, 1)
        return factor, inverse, correlations, slots, spare_slots
    return fn


def first_piece(arrived, basis_arrived):
    total = jnp.sum(arrived, axis=0)
    basis_total = jnp.sum(basis_arrived, axis=0)
    tile = total[BLOCK:]

    def moved(value):
        return roll(lane_range(value, 48, 64), -BLOCK, 1)

    sums = basis_arrived[:, 35, :] + moved(arrived[:, 18, :])
    shifted = moved(tile)
    every = basis_total[35:36] + shifted[2:3]
    images_sum = lane_range(tile, 48, 64)[3:4] + roll(lane_range(tile, 48, 64), BLOCK, 1)[4:5]
    lane = lanes_of(sums.shape)
    live = jnp.broadcast_to(sums[:, 80:81], sums.shape)
    whole = jnp.broadcast_to(every[:, 80:81], every.shape)
    scale = lax.rsqrt(whole)
    means = sums / live
    block_lane = (lane >= BASIS) & (lane < BASIS + BLOCK)
    weights = jnp.where(block_lane, means - every / whole, jnp.where(lane < BASIS, means, 0.0))
    column_mean = basis_total[32:33] / whole
    spread = basis_arrived[:, 32, :] - live * column_mean
    main = jnp.concatenate([basis_total[:BASIS], total[:BLOCK]], axis=0) + tm(weights, spread)[:48]
    spare = []
    spare_mean = []
    for k in range(2):
        mean = jnp.broadcast_to(basis_total[33 + k : 34 + k, 48:49], (1, TILE)) / whole
        column = jnp.broadcast_to(basis_arrived[:, 33 + k, 48:49], sums.shape) - live * mean
        known = lane_range(basis_total[33 + k : 34 + k], 0, BASIS) + shifted[k : k + 1]
        spare.append(known + jnp.sum(weights * column, axis=0, keepdims=True))
        spare_mean.append(mean)
    gram = jnp.concatenate([tile, roll(tile, -HALF, 1)], axis=0)
    between = tm(weights, jnp.where(lane < BASIS, sums, live * weights))[BASIS : BASIS + BLOCK]
    inner = gram + between
    scale16 = jnp.broadcast_to(scale, (BLOCK, TILE))
    coeffs = lane_range(inner, 0, BASIS) * scale16
    squares = lane_range(roll(inner, -BASIS, 1), 0, BLOCK) * scale16 * scale16
    folds = basis_total[40:48]
    basis_gram = jnp.concatenate([lane_range(roll(folds, -BASIS * n, 1), 0, BASIS) for n in range(4)], axis=0)
    correlations = at_rows(basis_gram, 0)
    combined = combination(coeffs, correlations)
    row8 = rows_of((8, TILE))
    both = lane_range(jnp.where(row8 == 0, spare[0], jnp.where(row8 == 1, spare[1], 0.0)), 0, 48) * scale
    slots = at_rows(main[:BASIS] * jnp.broadcast_to(scale, (BASIS, TILE)), 0)
    spare_slots = lane_range(both, 0, BASIS)
    block_main = main[BASIS:] * scale16 * scale16
    block_spare = lane_range(roll(both, -BASIS, 1), 0, BLOCK) * scale
    piece, rows = cleaned_piece(block_main, block_spare, combined, slots, spare_slots)
    lane8 = lanes_of((8, TILE))
    marks = jnp.where(row8 == 0, spare_mean[0], spare_mean[1])
    tail = jnp.where(row8 < 2, jnp.where(lane8 == BLOCK, marks, rows), jnp.where(row8 == 2, column_mean, 0.0))
    means8 = jnp.where(row8 == 0, column_mean, jnp.where(row8 == 1, spare_mean[0], jnp.where(row8 == 2, spare_mean[1], 0.0)))
    stats = jnp.where(row8 == 0, scale, jnp.where(row8 == 1, (every + images_sum) / whole, 0.0))
    message = copies(jnp.concatenate([piece, tail], axis=0))
    before = jnp.where(lanes_of((BLOCK, TILE)) == rows_of((BLOCK, TILE)), 1.0, 0.0)
    return message, squares, before, coeffs, combined, correlations, slots, spare_slots, piece, rows, means8, stats


def later_piece(arrived, inverse, known, correlations, slots, spare_slots, means8, stats):
    total = jnp.sum(arrived, axis=0)
    inner = inverse[:, :BLOCK]
    tile = total[BLOCK:]
    gram = jnp.concatenate([tile, roll(tile, -HALF, 1)], axis=0)
    coeffs = mm(inner, lane_range(gram, 0, BASIS)) + known
    squares = lane_range(roll(gram, -BASIS, 1), 0, BLOCK)
    combined = combination(coeffs, correlations)
    scale = stats[:1]
    rows = widened(mt(roll(tile, -48, 1)[:, :BLOCK], inner))
    row8 = rows_of((8, TILE))
    sums = jnp.broadcast_to(rows[2:3], (8, TILE))
    outer = tm(jnp.where(row8 == 0, sums, 0.0), jnp.where(row8 == 0, jnp.broadcast_to(means8[:1], (8, TILE)), 0.0))[:BLOCK]
    main = (mm(inner, total[:BLOCK]) - outer) * jnp.broadcast_to(scale, (BLOCK, TILE))
    spare_mean = jnp.where(row8 == 0, means8[1:2], jnp.where(row8 == 1, means8[2:3], 0.0))
    spare = jnp.where(row8 < 2, (rows - sums * spare_mean) * scale, 0.0)
    piece, fresh = cleaned_piece(main, spare, combined, slots, spare_slots)
    fresh = jnp.where(row8 < 2, fresh, 0.0)
    message = copies(jnp.concatenate([piece, fresh], axis=0))
    return message, squares, coeffs, combined, piece, fresh


def gathered(arrived):
    spare = jnp.concatenate([arrived[:, 16, :], arrived[:, 17, :], zeros(TILE - 2 * PIECES)], axis=0).T
    block = jnp.concatenate([arrived[p, :BLOCK] for p in range(PIECES)] + [lane_range(spare[:BLOCK], 0, HALF)], axis=1)
    return block, spare


def gene_sums(block, mean, core, weights, bases, chunk):
    pair = two(block)
    mean_pair = two(jnp.broadcast_to(mean, (BLOCK, LOCAL)))
    known = sum(b.shape[0] // 2 for b in bases)
    gap = jnp.zeros((80 - known, LOCAL), BF16)
    end = jnp.zeros((BLOCK, LOCAL), BF16)
    tops = [b[: b.shape[0] // 2] for b in bases] + ([gap] if known < 80 else []) + [pair[:BLOCK], mean_pair[:BLOCK], end]
    lows = [b[b.shape[0] // 2 :] for b in bases] + ([gap] if known < 80 else []) + [pair[BLOCK:], mean_pair[BLOCK:], end]
    gram = fine_mt(pair, jnp.concatenate(tops, axis=0), jnp.concatenate(lows, axis=0))
    image = stream_mt(pair, chunk) - gram[:, 96:97] * weights[:1]
    return near_message([halves(image), (lane_range(gram, 0, 96), None)], core)


def first_genes(arrived, core, weights, *rest):
    block, spare = gathered(arrived)
    mean = jnp.concatenate([arrived[p, 18:19] for p in range(PIECES)] + [lane_range(spare[BLOCK : BLOCK + 1], 0, HALF)], axis=1)
    return gene_sums(block, mean, core, weights, rest[:-1], rest[-1]), block, mean


def later_genes(arrived, mean, core, weights, *rest):
    block, _ = gathered(arrived)
    return gene_sums(block, mean, core, weights, rest[:-1], rest[-1]), block


def later_cells(arrived, before, correlations, images, weights, weighted, stats, chunk):
    total = jnp.sum(arrived, axis=0)
    inner = before[:, :BLOCK]
    image = mm(inner, jnp.concatenate([total[:BLOCK], total[BLOCK : 2 * BLOCK]], axis=1))
    gram = total[2 * BLOCK :]
    coeffs = mm(inner, lane_range(gram, 0, 80))
    squares = lane_range(roll(gram, -80, 1), 0, BLOCK)
    combined = combination(coeffs, correlations)
    block = image * stats[:1, :1] - mm(combined, images)
    sums = mt(jnp.broadcast_to(weights[:1], (8, 2 * TILE)), at_rows(block, 48))
    gram = mt(block, jnp.concatenate([weighted, block, zeros(80, 2 * TILE)], axis=0))
    rows = jnp.where(rows_of((8, TILE)) == 2, sums, 0.0)
    return block_message(stream_mm(two(block), chunk), gram, rows), squares, coeffs, combined, block


def cells_state(position):
    def fn(raw, before, coeffs, combined, correlations, images, expansions, block):
        squares = scaled(raw, before)
        factor, inverse, full, correlations = orthonormal(coeffs, combined, squares, correlations, position)
        block = mm(inverse[:, :BLOCK], block)
        images = images + at_rows(block, position)
        expansions = expansions + at_rows(combined + roll(factor, position, 1), position - BLOCK)
        return factor, inverse, mt(full, expansions), correlations, images, expansions, block
    return fn


def last_cells(arrived, before, correlations):
    gram = jnp.sum(arrived[:, 2 * BLOCK :], axis=0)
    coeffs = mm(before[:, :BLOCK], lane_range(gram, 0, 80))
    squares = scaled(roll(gram, -80, 1), before)
    combined = combination(coeffs, correlations)
    factor, inverse, _, _ = orthonormal(coeffs, combined, squares, correlations, BASIS + STEPS * BLOCK)
    return combined, factor, inverse


def first_images(image, stats, weights):
    scale = stats[:1, :1]
    both = image
    means = stats[1:2]
    means = jnp.concatenate([means[:, 48:80], means[:, BASIS : BASIS + BLOCK]], axis=1)
    column = at_rows(widened(jnp.broadcast_to(means, (8, 48))), 0).T[:48, :1]
    return (at_rows((both - column * weights[:1]) * scale, 0),)


def new_right(block, before, combined, inverse, *bases):
    known = sum(b.shape[0] // 2 for b in bases)
    high = jnp.concatenate([b[: b.shape[0] // 2] for b in bases], axis=0)
    low = jnp.concatenate([b[b.shape[0] // 2 :] for b in bases], axis=0)
    inner = inverse[:, :BLOCK]
    value = mm(mm(inner, before[:, :BLOCK]), block) - fine_mm(two(mm(inner, combined)[:, :known]), high, low)
    return value, two(value)


def new_left(block, combined, inverse, slots, position):
    value = mm(inverse[:, :BLOCK], block - mm(combined, slots))
    return value, slots + at_rows(value, position)


def far(value):
    return lax.all_to_all(value, FAR, split_axis=0, concat_axis=0, tiled=True)


def near(value):
    return lax.all_to_all(value, NEAR, split_axis=0, concat_axis=0, tiled=True)


def partner(value):
    return lax.ppermute(value, "core", [(0, 1), (1, 0)])


def own_genes(value, core):
    main = lax.dynamic_slice_in_dim(value, core * MAIN, MAIN, 1)
    spare = jnp.where(core == 0, value[:, 2 * MAIN : 2 * MAIN + HALF], value[:, 2 * MAIN + HALF :])
    return jnp.concatenate([main, jnp.pad(spare, ((0, 0), (0, HALF)))], axis=1)


def all_genes(own, other, core):
    first = jnp.where(core == 0, own, other)
    second = jnp.where(core == 0, other, own)
    return jnp.concatenate([first[:, :MAIN], second[:, :MAIN], first[:, MAIN : MAIN + HALF], second[:, MAIN : MAIN + HALF]], axis=1)


def body(counts, live_rows, left_basis, right_basis, right_start):
    core = lax.axis_index("core")
    core_index = jnp.full((8, TILE), core, jnp.int32)
    live = live_rows[0]
    sent = own_genes(counts, 1 - core)
    got = partner(sent)
    cells = jnp.arange(ROWS, dtype=jnp.int32)
    weight = (cells < live).astype(F32)
    bundle = jnp.concatenate([left_basis, jnp.broadcast_to(weight, (8, ROWS))], axis=0)
    got_bundle = partner(bundle)
    weights = jnp.concatenate([bundle[BASIS:], got_bundle[BASIS:]], axis=1)
    basis_left = jnp.concatenate([left_basis, got_bundle[:BASIS]], axis=1)
    every = jnp.concatenate([own_genes(counts, core), got], axis=0)
    logged = jnp.where(weights[0][:, None] > 0, jnp.log1p(every.astype(F32)), 0.0)
    top = lax.reduce_precision(logged, 8, 7)
    high, low = top.astype(BF16), (logged - top).astype(BF16)
    basis_right = own_genes(right_basis, core)
    start = own_genes(right_start, core)

    square = ((TILE, TILE), F32)
    slim = ((BLOCK, TILE), F32)
    small = ((8, TILE), F32)
    wide = ((BLOCK, 2 * TILE), F32)
    tall = ((TILE, 2 * TILE), F32)
    long = ((BLOCK, LOCAL), F32)
    row = ((1, LOCAL), F32)
    count = BASIS + BLOCK

    matrix = (high, low)
    basis_message, weighted = call(
        basis_cells, "basis_cells", [((PIECES, 48, TILE), F32), ((BASIS, 2 * TILE), F32)],
        weights, basis_left, streams=matrix)
    basis_arrived = far(basis_message)
    basis_message, basis_right = lax.optimization_barrier((basis_message, basis_right))
    own_sums, other_sums, lead = call(
        start_kernel, "start", [((3 * count, TILE), F32), ((3 * count, TILE), F32), ((2 * count, LOCAL), BF16)],
        basis_right, start, streams=matrix)
    bases = [lead]
    chip_sums = own_sums + partner(other_sums)
    arrived = jnp.stack([chip_sums] + [lax.ppermute(chip_sums, "x", [(i, (i + k) % 4) for i in range(4)]) for k in (1, 2, 3)])
    message, image, right_corr = call(
        first_cells, "first_cells", [((PIECES, 24, TILE), F32), ((count, 2 * TILE), F32), square],
        arrived, weights, weighted, streams=matrix, arrived=True)
    message, basis_arrived = lax.optimization_barrier((message, basis_arrived))
    arrived = far(message)
    lefts, rights, diags, couples = [], [], [], []
    left_slots = jnp.pad(weighted, ((0, TILE - BASIS), (0, 0)))
    expansions = jnp.zeros((TILE, TILE), F32)
    piece_message = ((PIECES, 24, TILE), F32)
    gene_message = ((PEERS, 3 * BLOCK, TILE), F32)
    for step in range(STEPS):
        position = BASIS + step * BLOCK
        if step == 0:
            message, raw, right_inverse, coeffs, combined, left_corr, slots, spare_slots, piece, rows, means8, stats = call(
                first_piece, "first_piece",
                [piece_message, slim, slim, slim, slim, square, square, small, slim, small, small, small], arrived, basis_arrived, arrived=2)
        else:
            message, raw, coeffs, combined, piece, rows = call(
                later_piece, "piece", [piece_message, slim, slim, slim, slim, small],
                arrived, right_inverse, known, left_corr, slots, spare_slots, means8, stats, arrived=True)
        arrived = far(message)
        factor, left_inverse, left_corr, slots, spare_slots = call(
            piece_state(position), "piece_state", [slim, slim, square, square, small],
            raw, right_inverse, coeffs, combined, left_corr, slots, spare_slots, piece, rows)
        diags.append(factor[:, :BLOCK])
        if step == 0:
            (images,) = call(first_images, "first_images", [tall], image, stats, weights)
            block = images[BASIS : BASIS + BLOCK]
        left, left_slots = call(
            lambda a, b, c, d, position=position: new_left(a, b, c, d, position), "new_left", [wide, tall],
            block, combined, left_inverse, left_slots)
        lefts.append(left[:, :ROWS])
        arrived, left_inverse, left_corr, slots, spare_slots, images = lax.optimization_barrier(
            (arrived, left_inverse, left_corr, slots, spare_slots, images))
        if step == 0:
            message, genes_block, mean = call(first_genes, "first_genes", [gene_message, long, row],
                                              arrived, core_index, weights, *bases, streams=matrix, arrived=True)
        else:
            message, genes_block = call(later_genes, "genes", [gene_message, long],
                                        arrived, mean, core_index, weights, *bases, streams=matrix, arrived=True)
        arrived = near(message)
        if step + 1 < STEPS:
            message, raw, coeffs, combined, block = call(
                later_cells, "cells", [piece_message, slim, slim, slim, wide],
                arrived, left_inverse, right_corr, images, weights, weighted, stats, streams=matrix, arrived=True)
            arrived = far(message)
            factor, right_inverse, known, right_corr, images, expansions, block = call(
                cells_state(position + BLOCK), "cells_state", [slim, slim, slim, square, tall, square, wide],
                raw, left_inverse, coeffs, combined, right_corr, images, expansions, block)
        else:
            combined, factor, right_inverse = call(
                last_cells, "last_cells", [slim, slim, slim], arrived, left_inverse, right_corr, arrived=True)
        couples.append(factor[:, :BLOCK])
        value, pair = call(new_right, "new_right", [long, ((2 * BLOCK, LOCAL), BF16)],
                           genes_block, left_inverse, combined, right_inverse, *bases)
        bases = bases + [pair]
        rights.append(all_genes(value, partner(value), core))
    left_vectors = jnp.concatenate(lefts, axis=0) * math.sqrt(8192.0)
    right_vectors = jnp.concatenate(rights, axis=0) * math.sqrt(33280.0)
    return left_vectors, right_vectors, jnp.stack(diags), jnp.stack(couples)


def solution(mesh):
    split = Mesh(mesh.devices.reshape(8, 4, 2, 4), ("z", "y", "core", "x"))
    cells = ("z", "y", "core")
    return jax.shard_map(
        body,
        mesh=split,
        in_specs=(P(cells, "x"), P(cells), P(None, cells), P(None, "x"), P(None, "x")),
        out_specs=(P(None, cells), P(None, "x"), P(), P()),
        check_vma=False,
    )
```

```python
import inspect
import math

import jax
import jax.numpy as jnp
from jax import lax
from jax.experimental import pallas as pl
from jax.experimental.pallas import tpu as pltpu
from jax.sharding import Mesh
from jax.sharding import PartitionSpec as P

BASIS = 32
BLOCK = 16
STEPS = 3
ROWS = 128
TILE = 128
PIECES = 32
PEERS = 8
MAIN = PIECES * TILE
LOCAL = MAIN + TILE
CHUNKS = 3
SMALL = 50000
CHUNK = LOCAL // CHUNKS
HALF = TILE // 2
FAR = ("z", "y")
NEAR = ("core", "x")
F32 = jnp.float32
BF16 = jnp.bfloat16


def in_hbm(value):
    return pltpu.with_memory_space_constraint(value, pltpu.HBM)


def is_small(shape):
    return math.prod(shape) <= SMALL


def call(fn, name, outs, *args, streams=(), arrived=False, late_args=False):
    held = [is_small(a.shape) or n < int(arrived) for n, a in enumerate(args)]
    args = [a if h else in_hbm(a) for a, h in zip(args, held)]
    whole = list(streams[:1])
    streams = [in_hbm(a) for a in streams[1:]]
    count, kept, given = len(args), len(streams), len(outs)
    first = len(whole)
    loaded = [n for n in range(count) if not held[n]]
    stored = [n for n in range(given) if not is_small(outs[n][0])]
    total = len(loaded) + 2 * len(stored) + kept * CHUNKS

    def kernel(*refs):
        operands = refs[:count]
        resident = refs[count : count + first]
        sources = refs[count + first : count + first + kept]
        results = refs[count + first + kept : count + first + kept + given]
        scratch = refs[count + first + kept + given :]
        inside = scratch[: len(loaded)]
        written = scratch[len(loaded) : len(loaded) + len(stored)]
        parts = scratch[len(loaded) + len(stored) : len(loaded) + len(stored) + kept]
        semaphores = scratch[-1] if total else None
        entering = [pltpu.make_async_copy(operands[n], inside[m], semaphores.at[m]) for m, n in enumerate(loaded)]
        base = len(loaded) + 2 * len(stored)
        streaming = []
        for k in range(CHUNKS):
            window = (slice(None), pl.ds(k * CHUNK, CHUNK))
            streaming.append([
                pltpu.make_async_copy(source.at[window], parts[n].at[window], semaphores.at[base + n * CHUNKS + k])
                for n, source in enumerate(sources)
            ])
        first_copies = [copy for group in streaming for copy in group]
        for copy in first_copies + entering if late_args else entering + first_copies:
            copy.start()

        def chunk(k):
            for copy in streaming[k]:
                copy.wait()
            return [ref[:, k * CHUNK : (k + 1) * CHUNK] for ref in (*resident, *parts)]

        def late(m):
            def get():
                entering[m].wait()
                return inside[m][...]
            return get

        values = [operands[n][...] if held[n] else late(loaded.index(n)) for n in range(count)]
        leaving = []
        made = fn(*values, chunk) if kept else fn(*values)
        for n, value in made if inspect.isgenerator(made) else enumerate(made):
            if n not in stored:
                results[n][...] = value
                continue
            place = written[stored.index(n)]
            begin, value = value if isinstance(value, tuple) else (0, value)
            window = pl.ds(begin, value.shape[0])
            place[begin : begin + value.shape[0]] = value
            semaphore = semaphores.at[len(loaded) + 2 * stored.index(n) + (begin > 0)]
            copy = pltpu.make_async_copy(place.at[window], results[n].at[window], semaphore)
            copy.start()
            leaving.append(copy)
        for copy in leaving:
            copy.wait()

    vmem = pl.BlockSpec(memory_space=pltpu.VMEM)
    hbm = pl.BlockSpec(memory_space=pltpu.HBM)
    scratch_shapes = [pltpu.VMEM(args[n].shape, args[n].dtype) for n in loaded]
    scratch_shapes += [pltpu.VMEM(*outs[n]) for n in stored]
    scratch_shapes += [pltpu.VMEM(a.shape, a.dtype) for a in streams]
    if total:
        scratch_shapes.append(pltpu.SemaphoreType.DMA((total,)))
    return pl.pallas_call(
        kernel,
        out_shape=[pltpu.HBM(s, d) if n in stored else jax.ShapeDtypeStruct(s, d) for n, (s, d) in enumerate(outs)],
        in_specs=[vmem if h else hbm for h in held] + [vmem] * first + [hbm] * kept,
        out_specs=[hbm if n in stored else vmem for n in range(given)],
        scratch_shapes=scratch_shapes,
        compiler_params=pltpu.CompilerParams(vmem_limit_bytes=32 * 1024 * 1024),
        name=name,
    )(*args, *whole, *streams)


def roll(value, shift, axis):
    size = value.shape[axis]
    return pltpu.roll(value, shift % size, axis)


def mm(lhs, rhs):
    return lax.dot_general(lhs, rhs, (((1,), (0,)), ((), ())), precision=lax.Precision.HIGHEST, preferred_element_type=F32)


def mt(lhs, rhs):
    return lax.dot_general(lhs, rhs, (((1,), (1,)), ((), ())), precision=lax.Precision.HIGHEST, preferred_element_type=F32)


def tm(lhs, rhs):
    return lax.dot_general(lhs, rhs, (((0,), (0,)), ((), ())), precision=lax.Precision.HIGHEST, preferred_element_type=F32)


def two(value):
    high = value.astype(BF16)
    return jnp.concatenate([high, (value - high.astype(F32)).astype(BF16)], axis=0)


def folded(value):
    half = value.shape[0] // 2
    return value[:half] + value[half:]


def fine_mt(pair, high, low):
    dims = (((1,), (1,)), ((), ()))
    return folded(
        lax.dot_general(pair, high, dims, preferred_element_type=F32)
        + lax.dot_general(pair, low, dims, preferred_element_type=F32)
    )


def fine_mm(pair, high, low):
    dims = (((1,), (0,)), ((), ()))
    return folded(
        lax.dot_general(pair, high, dims, preferred_element_type=F32)
        + lax.dot_general(pair, low, dims, preferred_element_type=F32)
    )


def stream_mt(pair, chunk):
    dims = (((1,), (1,)), ((), ()))
    total = None
    for k in range(CHUNKS):
        part = pair[:, k * CHUNK : (k + 1) * CHUNK]
        for matrix in chunk(k):
            one = lax.dot_general(part, matrix, dims, preferred_element_type=F32)
            total = one if total is None else total + one
    return folded(total)


def stream_mm(pair, chunk):
    dims = (((1,), (0,)), ((), ()))
    parts = []
    for k in range(CHUNKS):
        high, low = chunk(k)
        parts.append(
            folded(
                lax.dot_general(pair, high, dims, preferred_element_type=F32)
                + lax.dot_general(pair, low, dims, preferred_element_type=F32)
            )
        )
    return jnp.concatenate(parts, axis=1)


def zeros(rows, lanes=TILE, dtype=F32):
    return jnp.zeros((rows, lanes), dtype)


def at_rows(value, start, rows=TILE):
    count, lanes = value.shape
    parts = []
    if start:
        parts.append(zeros(start, lanes, value.dtype))
    parts.append(value)
    if start + count < rows:
        parts.append(zeros(rows - start - count, lanes, value.dtype))
    return jnp.concatenate(parts, axis=0)


def lanes_of(shape):
    return lax.broadcasted_iota(jnp.int32, shape, 1)


def rows_of(shape):
    return lax.broadcasted_iota(jnp.int32, shape, 0)


def lane_range(value, start, stop):
    lane = lanes_of(value.shape)
    return jnp.where((lane >= start) & (lane < stop), value, 0.0)


def widened(value):
    return jnp.concatenate([value, zeros(value.shape[0], TILE - value.shape[1])], axis=1)


def factored(squares):
    lane = lanes_of((BLOCK, TILE))
    row = rows_of((BLOCK, TILE))
    work = squares + jnp.where(lane == row + BLOCK, 1.0, 0.0)
    factor = jnp.zeros((BLOCK, TILE), F32)
    for k in range(BLOCK):
        column = jnp.broadcast_to(work[:, k : k + 1], (BLOCK, TILE))
        scale = 1.0 / jnp.sqrt(jnp.broadcast_to(column[k : k + 1], (BLOCK, TILE)))
        column = column * scale
        pivot = work[k : k + 1] * scale
        factor = jnp.where((lane == k) & (row >= k), column, factor)
        work = jnp.where(row > k, work - column * pivot, jnp.where(row == k, pivot, work))
    return factor, lane_range(work, BLOCK, 2 * BLOCK)


def combination(coeffs, correlations):
    return coeffs + coeffs - mm(coeffs, correlations)


def scaled(raw, inverse):
    inner = inverse[:, :BLOCK]
    return widened(mt(mm(inner, raw[:, :BLOCK]), inner))


def orthonormal(coeffs, combined, squares, correlations, position):
    passed = mm(combined, correlations)
    remaining = squares + widened(mt(passed - coeffs, combined) - mt(combined, coeffs))
    factor, shifted = factored(remaining)
    inverse = lane_range(roll(shifted, -BLOCK, 1), 0, BLOCK)
    residual = mm(inverse[:, :BLOCK], coeffs - passed)
    identity = jnp.where(lanes_of((BLOCK, TILE)) == rows_of((BLOCK, TILE)) + position, 1.0, 0.0)
    full = residual + identity
    if position + BLOCK <= TILE:
        placed = at_rows(residual, position)
        correlations = correlations + placed + placed.T + at_rows(identity, position)
    return factor, inverse, full, correlations


def tiles(value, start, rows):
    return [value[start : start + rows, p * TILE : (p + 1) * TILE] for p in range(PIECES)]


def near_blocks(parts, core):
    blocks = []
    for target in range(2):
        same = core[0, 0] == target
        rows = []
        for a, b in parts:
            if b is None:
                rows.append(a)
            else:
                rows += [jnp.where(same, a, b), jnp.where(same, b, a)]
        blocks.append(jnp.concatenate(rows, axis=0))
    return blocks


def near_message(parts, core):
    blocks = near_blocks(parts, core)
    return jnp.stack([blocks[n // (PEERS // 2)] for n in range(PEERS)])


def halves(value):
    return value[:, :TILE], value[:, TILE:]


def start_kernel(tied, basis, block, chunk):
    lead = two(jnp.concatenate([basis(), block()], axis=0))
    yield 2, lead
    image = stream_mt(lead, chunk)
    count = BASIS + BLOCK
    gram = fine_mt(lead, jnp.concatenate([lead[:count], jnp.zeros((TILE - count, LOCAL), BF16)], axis=0),
                   jnp.concatenate([lead[count:], jnp.zeros((TILE - count, LOCAL), BF16)], axis=0))
    own, other = halves(image)
    yield 0, jnp.concatenate([own, other, gram], axis=0)
    yield 1, jnp.concatenate([other, own, gram], axis=0)


def basis_cells(weights, left_basis, chunk):
    weight = weights[:1]
    weighted = left_basis * weight
    ones = jnp.broadcast_to(weight, (8, weight.shape[1]))
    sums = mt(ones, jnp.concatenate([weighted, zeros(48, 2 * TILE), ones, zeros(TILE - 88, 2 * TILE)], axis=0))
    live = jnp.sum(weight, axis=1, keepdims=True)
    centred = weighted - jnp.sum(weighted, axis=1, keepdims=True) / live * weight
    lead = jnp.concatenate([centred, zeros(BLOCK, 2 * TILE), ones, zeros(8, 2 * TILE)], axis=0)
    product = stream_mm(two(lead), chunk)
    spare = jnp.concatenate([product[:, MAIN:], zeros(TILE - 64)], axis=0).T
    gram = mt(weighted, at_rows(weighted, 0))
    folds = gram[:8]
    for n in range(1, 4):
        folds = folds + roll(gram[8 * n : 8 * n + 8], BASIS * n, 1)
    row = rows_of((8, TILE))
    pieces = []
    for p in range(PIECES):
        main = product[:, p * TILE : (p + 1) * TILE]
        tail = jnp.where(row == 0, main[48:56], 0.0)
        tail = jnp.where(row == 1, spare[p : p + 1], tail)
        tail = jnp.where(row == 2, spare[PIECES + p : PIECES + p + 1], tail)
        tail = jnp.where(row == 3, sums, tail)
        pieces.append(jnp.concatenate([main[:BASIS], tail, folds], axis=0))
    return jnp.stack(pieces), weighted


def block_message(product, gram, rows):
    spare = at_rows(product[:, MAIN:], 48).T
    row8 = rows_of((8, TILE))
    tile = gram[:8] + roll(gram[8:], HALF, 1) + rows
    pieces = []
    for p in range(PIECES):
        tail = tile + jnp.where(row8 == 0, spare[p : p + 1], jnp.where(row8 == 1, spare[PIECES + p : PIECES + p + 1], 0.0))
        pieces.append(jnp.concatenate([product[:, p * TILE : (p + 1) * TILE], tail], axis=0))
    return jnp.stack(pieces)


def first_cells(arrived, weights, weighted, chunk):
    total = jnp.sum(arrived, axis=0)
    count = BASIS + BLOCK
    image = jnp.concatenate([total[:count], total[count : 2 * count]], axis=1)
    correlations = at_rows(total[2 * count :], 0)
    weight = weights[:1]
    block = image[BASIS:]
    ones = jnp.broadcast_to(weight, (8, weight.shape[1]))
    row8 = rows_of((8, TILE))
    rows = jnp.where(row8 == 2, mt(ones, at_rows(block, 48)), 0.0)
    for n in range(2):
        rows = rows + jnp.where(row8 == 3 + n, mt(ones, at_rows(image[BLOCK * n : BLOCK * n + BLOCK], 48)), 0.0)
    live = jnp.sum(weight, axis=1, keepdims=True)
    centred = block - jnp.sum(block, axis=1, keepdims=True) / live * weight
    gram = mt(centred, jnp.concatenate([weighted, centred, zeros(80, 2 * TILE)], axis=0))
    return block_message(stream_mm(two(centred), chunk), gram, rows), image, correlations


def copies(block):
    return jnp.concatenate([block] * PIECES, axis=0)


def cleaned_piece(main, spare, combined, slots, spare_slots):
    return main - mm(combined, slots), widened(spare[:, :BLOCK] - mt(spare_slots, combined))


def spare_line(rows):
    return rows[:1] + roll(rows[1:2], BASIS, 1)


def piece_state(position):
    def fn(raw, before, coeffs, combined, correlations, slots, spare_slots, piece, rows):
        squares = scaled(raw, before)
        factor, inverse, _, correlations = orthonormal(coeffs, combined, squares, correlations, position)
        inner = inverse[:, :BLOCK]
        slots = slots + at_rows(mm(inner, piece), position)
        spare_slots = spare_slots + roll(widened(mt(rows[:, :BLOCK], inner)), position, 1)
        return factor, inverse, correlations, slots, spare_slots
    return fn


def first_piece(arrived, basis_arrived):
    total = jnp.sum(arrived, axis=0)
    basis_total = jnp.sum(basis_arrived, axis=0)
    tile = total[BLOCK:]

    def moved(value):
        return roll(lane_range(value, 48, 64), -BLOCK, 1)

    sums = basis_arrived[:, 35, :] + moved(arrived[:, 18, :])
    shifted = moved(tile)
    every = basis_total[35:36] + shifted[2:3]
    images_sum = lane_range(tile, 48, 64)[3:4] + roll(lane_range(tile, 48, 64), BLOCK, 1)[4:5]
    lane = lanes_of(sums.shape)
    live = jnp.broadcast_to(sums[:, 80:81], sums.shape)
    whole = jnp.broadcast_to(every[:, 80:81], every.shape)
    scale = lax.rsqrt(whole)
    means = sums / live
    block_lane = (lane >= BASIS) & (lane < BASIS + BLOCK)
    weights = jnp.where(block_lane, means - every / whole, jnp.where(lane < BASIS, means, 0.0))
    column_mean = basis_total[32:33] / whole
    spread = basis_arrived[:, 32, :] - live * column_mean
    main = jnp.concatenate([basis_total[:BASIS], total[:BLOCK]], axis=0) + tm(weights, spread)[:48]
    spare = []
    spare_mean = []
    for k in range(2):
        mean = jnp.broadcast_to(basis_total[33 + k : 34 + k, 48:49], (1, TILE)) / whole
        column = jnp.broadcast_to(basis_arrived[:, 33 + k, 48:49], sums.shape) - live * mean
        known = lane_range(basis_total[33 + k : 34 + k], 0, BASIS) + shifted[k : k + 1]
        spare.append(known + jnp.sum(weights * column, axis=0, keepdims=True))
        spare_mean.append(mean)
    gram = jnp.concatenate([tile, roll(tile, -HALF, 1)], axis=0)
    between = tm(weights, jnp.where(lane < BASIS, sums, live * weights))[BASIS : BASIS + BLOCK]
    inner = gram + between
    scale16 = jnp.broadcast_to(scale, (BLOCK, TILE))
    coeffs = lane_range(inner, 0, BASIS) * scale16
    squares = lane_range(roll(inner, -BASIS, 1), 0, BLOCK) * scale16 * scale16
    folds = basis_total[40:48]
    basis_gram = jnp.concatenate([lane_range(roll(folds, -BASIS * n, 1), 0, BASIS) for n in range(4)], axis=0)
    correlations = at_rows(basis_gram, 0)
    combined = combination(coeffs, correlations)
    row8 = rows_of((8, TILE))
    both = lane_range(jnp.where(row8 == 0, spare[0], jnp.where(row8 == 1, spare[1], 0.0)), 0, 48) * scale
    slots = at_rows(main[:BASIS] * jnp.broadcast_to(scale, (BASIS, TILE)), 0)
    spare_slots = lane_range(both, 0, BASIS)
    block_main = main[BASIS:] * scale16 * scale16
    block_spare = lane_range(roll(both, -BASIS, 1), 0, BLOCK) * scale
    piece, rows = cleaned_piece(block_main, block_spare, combined, slots, spare_slots)
    lane1 = lanes_of((1, TILE))
    tail = spare_line(rows)
    for k in range(2):
        tail = jnp.where(lane1 == BASIS * k + BLOCK, spare_mean[k], tail)
    means8 = jnp.where(row8 == 0, column_mean, jnp.where(row8 == 1, spare_mean[0], jnp.where(row8 == 2, spare_mean[1], 0.0)))
    stats = jnp.where(row8 == 0, scale, jnp.where(row8 == 1, (every + images_sum) / whole, 0.0))
    message = copies(jnp.concatenate([piece, tail, column_mean], axis=0))
    before = jnp.where(lanes_of((BLOCK, TILE)) == rows_of((BLOCK, TILE)), 1.0, 0.0)
    return message, squares, before, coeffs, combined, correlations, slots, spare_slots, piece, rows, means8, stats


def later_piece(arrived, inverse, known, correlations, slots, spare_slots, means8, stats):
    total = jnp.sum(arrived, axis=0)
    inner = inverse[:, :BLOCK]
    tile = total[BLOCK:]
    gram = jnp.concatenate([tile, roll(tile, -HALF, 1)], axis=0)
    coeffs = mm(inner, lane_range(gram, 0, BASIS)) + known
    squares = lane_range(roll(gram, -BASIS, 1), 0, BLOCK)
    combined = combination(coeffs, correlations)
    scale = stats[:1]
    rows = widened(mt(roll(tile, -48, 1)[:, :BLOCK], inner))
    row8 = rows_of((8, TILE))
    sums = jnp.broadcast_to(rows[2:3], (8, TILE))
    outer = tm(jnp.where(row8 == 0, sums, 0.0), jnp.where(row8 == 0, jnp.broadcast_to(means8[:1], (8, TILE)), 0.0))[:BLOCK]
    main = (mm(inner, total[:BLOCK]) - outer) * jnp.broadcast_to(scale, (BLOCK, TILE))
    spare_mean = jnp.where(row8 == 0, means8[1:2], jnp.where(row8 == 1, means8[2:3], 0.0))
    spare = jnp.where(row8 < 2, (rows - sums * spare_mean) * scale, 0.0)
    piece, fresh = cleaned_piece(main, spare, combined, slots, spare_slots)
    fresh = jnp.where(row8 < 2, fresh, 0.0)
    message = copies(jnp.concatenate([piece, spare_line(fresh)], axis=0))
    return message, squares, coeffs, combined, piece, fresh


def gathered(arrived):
    size = arrived.shape[0] // PIECES
    lines = jnp.concatenate([arrived[p * size + BLOCK : p * size + BLOCK + 1] for p in range(PIECES)], axis=0)
    spare = jnp.concatenate([lines, roll(lines, -BASIS, 1), zeros(TILE - 2 * PIECES)], axis=0).T
    block = jnp.concatenate(
        [arrived[p * size : p * size + BLOCK] for p in range(PIECES)] + [lane_range(spare[:BLOCK], 0, HALF)], axis=1)
    return block, spare


def gene_gram(pair, mean, bases):
    mean_pair = two(jnp.broadcast_to(mean, (BLOCK, LOCAL)))
    bases = [b() for b in bases]
    known = sum(b.shape[0] // 2 for b in bases)
    gap = jnp.zeros((80 - known, LOCAL), BF16)
    end = jnp.zeros((BLOCK, LOCAL), BF16)
    tops = [b[: b.shape[0] // 2] for b in bases] + ([gap] if known < 80 else []) + [pair[:BLOCK], mean_pair[:BLOCK], end]
    lows = [b[b.shape[0] // 2 :] for b in bases] + ([gap] if known < 80 else []) + [pair[BLOCK:], mean_pair[BLOCK:], end]
    return fine_mt(pair, jnp.concatenate(tops, axis=0), jnp.concatenate(lows, axis=0))


def gene_sums(pair, mean, core, weights, bases, chunk):
    image = stream_mt(pair, chunk)
    gram = gene_gram(pair, mean, bases)
    image = image - gram[:, 96:97] * weights[:1]
    return near_message([halves(image), (lane_range(gram, 0, 96), None)], core)


def first_genes(arrived, core, weights, *rest):
    block, spare = gathered(arrived)
    yield 1, block
    mean = jnp.concatenate(
        [arrived[18 * p + 17 : 18 * p + 18] for p in range(PIECES)] + [lane_range(spare[BLOCK : BLOCK + 1], 0, HALF)], axis=1)
    yield 2, mean
    yield 0, gene_sums(two(block), mean, core, weights, rest[:-1], rest[-1])


def later_genes(arrived, mean, core, weights, *rest):
    block, _ = gathered(arrived)
    yield 1, block
    yield 0, gene_sums(two(block), mean, core, weights, rest[:-1], rest[-1])


def last_genes(arrived, *bases):
    block, _ = gathered(arrived)
    yield 1, block
    gram = lane_range(gene_gram(two(block), zeros(1, LOCAL), bases), 0, 96)
    yield 0, jnp.stack([gram] * PEERS)


def later_cells(arrived, before, correlations, images, weights, weighted, stats, chunk):
    total = jnp.sum(arrived, axis=0)
    inner = before[:, :BLOCK]
    image = mm(inner, jnp.concatenate([total[:BLOCK], total[BLOCK : 2 * BLOCK]], axis=1))
    gram = total[2 * BLOCK :]
    coeffs = mm(inner, lane_range(gram, 0, 80))
    squares = lane_range(roll(gram, -80, 1), 0, BLOCK)
    combined = combination(coeffs, correlations)
    block = image * stats[:1, :1] - mm(combined, images)
    sums = mt(jnp.broadcast_to(weights[:1], (8, 2 * TILE)), at_rows(block, 48))
    gram = mt(block, jnp.concatenate([weighted, block, zeros(80, 2 * TILE)], axis=0))
    rows = jnp.where(rows_of((8, TILE)) == 2, sums, 0.0)
    return block_message(stream_mm(two(block), chunk), gram, rows), squares, coeffs, combined, block


def cells_state(position):
    def fn(raw, before, coeffs, combined, correlations, images, expansions, block):
        squares = scaled(raw, before)
        factor, inverse, full, correlations = orthonormal(coeffs, combined, squares, correlations, position)
        block = mm(inverse[:, :BLOCK], block)
        images = images + at_rows(block, position)
        expansions = expansions + at_rows(combined + roll(factor, position, 1), position - BLOCK)
        return factor, inverse, mt(full, expansions), correlations, images, expansions, block
    return fn


def last_step(arrived, before, correlations, first_factor, second_factor, block, basis, start, first, second):
    size = math.sqrt(33280.0)
    gram = jnp.sum(arrived, axis=0)
    coeffs = mm(before[:, :BLOCK], lane_range(gram, 0, 80))
    squares = scaled(roll(gram, -80, 1), before)
    combined = combination(coeffs, correlations)
    factor, inverse, _, _ = orthonormal(coeffs, combined, squares, correlations, BASIS + STEPS * BLOCK)
    inner = inverse[:, :BLOCK]
    first, second = first(), second()
    yield 0, (0, jnp.concatenate([first, second], axis=0) * size)
    slots = jnp.concatenate([basis(), start(), first, second], axis=0)
    high = slots.astype(BF16)
    low = (slots - high.astype(F32)).astype(BF16)
    value = mm(mm(inner, before[:, :BLOCK]), block()) - fine_mm(two(mm(inner, combined)[:, :80]), high, low)
    yield 0, (2 * BLOCK, value * size)
    yield 1, jnp.stack([first_factor[:, :BLOCK], second_factor[:, :BLOCK], factor[:, :BLOCK]])


def first_images(image, stats, weights):
    scale = stats[:1, :1]
    both = image
    means = stats[1:2]
    means = jnp.concatenate([means[:, 48:80], means[:, BASIS : BASIS + BLOCK]], axis=1)
    column = at_rows(widened(jnp.broadcast_to(means, (8, 48))), 0).T[:48, :1]
    return (at_rows((both - column * weights[:1]) * scale, 0),)


def new_right(block, before, combined, inverse, *bases):
    bases = [b() for b in bases]
    known = sum(b.shape[0] // 2 for b in bases)
    high = jnp.concatenate([b[: b.shape[0] // 2] for b in bases], axis=0)
    low = jnp.concatenate([b[b.shape[0] // 2 :] for b in bases], axis=0)
    inner = inverse[:, :BLOCK]
    value = mm(mm(inner, before[:, :BLOCK]), block()) - fine_mm(two(mm(inner, combined)[:, :known]), high, low)
    return value, two(value)


def new_left(block, combined, inverse, slots, position):
    value = mm(inverse[:, :BLOCK], block - mm(combined, slots))
    return value, slots + at_rows(value, position)


def gather(value):
    size = value.shape[0] // PIECES * TILE
    return far(value.reshape(PIECES, 1, size)).reshape(value.shape)


def far(value):
    return lax.all_to_all(value, FAR, split_axis=0, concat_axis=0, tiled=True)


def near(value):
    return lax.all_to_all(value, NEAR, split_axis=0, concat_axis=0, tiled=True)


def partner(value):
    return lax.ppermute(value, "core", [(0, 1), (1, 0)])


def own_genes(value, core):
    main = lax.dynamic_slice_in_dim(value, core * MAIN, MAIN, 1)
    spare = jnp.where(core == 0, value[:, 2 * MAIN : 2 * MAIN + HALF], value[:, 2 * MAIN + HALF :])
    return jnp.concatenate([main, jnp.pad(spare, ((0, 0), (0, HALF)))], axis=1)


def all_genes(own, other, core):
    first = jnp.where(core == 0, own, other)
    second = jnp.where(core == 0, other, own)
    return jnp.concatenate([first[:, :MAIN], second[:, :MAIN], first[:, MAIN : MAIN + HALF], second[:, MAIN : MAIN + HALF]], axis=1)


def body(counts, live_rows, left_basis, right_basis, right_start):
    core = lax.axis_index("core")
    core_index = jnp.full((8, TILE), core, jnp.int32)
    live = live_rows[0]
    sent = own_genes(counts, 1 - core)
    got = partner(sent)
    cells = jnp.arange(ROWS, dtype=jnp.int32)
    weight = (cells < live).astype(F32)
    bundle = jnp.concatenate([left_basis, jnp.broadcast_to(weight, (8, ROWS))], axis=0)
    got_bundle = partner(bundle)
    weights = jnp.concatenate([bundle[BASIS:], got_bundle[BASIS:]], axis=1)
    basis_left = jnp.concatenate([left_basis, got_bundle[:BASIS]], axis=1)
    every = jnp.concatenate([own_genes(counts, core), got], axis=0)
    logged = jnp.where(weights[0][:, None] > 0, jnp.log(1.0 + every.astype(F32)), 0.0)
    top = lax.reduce_precision(logged, 8, 7)
    high, low = top.astype(BF16), (logged - top).astype(BF16)
    basis_right = own_genes(right_basis, core)
    start = own_genes(right_start, core)

    square = ((TILE, TILE), F32)
    slim = ((BLOCK, TILE), F32)
    small = ((8, TILE), F32)
    wide = ((BLOCK, 2 * TILE), F32)
    tall = ((TILE, 2 * TILE), F32)
    long = ((BLOCK, LOCAL), F32)
    row = ((1, LOCAL), F32)
    count = BASIS + BLOCK

    matrix = (high, low)
    basis_message, weighted = call(
        basis_cells, "basis_cells", [((PIECES, 48, TILE), F32), ((BASIS, 2 * TILE), F32)],
        weights, basis_left, streams=matrix)
    basis_arrived = far(basis_message)
    basis_message, tied = lax.optimization_barrier((basis_message, weights))
    own_sums, other_sums, lead = call(
        start_kernel, "start", [((3 * count, TILE), F32), ((3 * count, TILE), F32), ((2 * count, LOCAL), BF16)],
        tied, basis_right, start, streams=matrix)
    bases = [lead]
    chip_sums = own_sums + partner(other_sums)
    arrived = jnp.stack([chip_sums] + [lax.ppermute(chip_sums, "x", [(i, (i + k) % 4) for i in range(4)]) for k in (1, 2, 3)])
    message, image, right_corr = call(
        first_cells, "first_cells", [((PIECES, 24, TILE), F32), ((count, 2 * TILE), F32), square],
        arrived, weights, weighted, streams=matrix, arrived=True)
    message, basis_arrived = lax.optimization_barrier((message, basis_arrived))
    arrived = far(message)
    lefts, rights, diags, couples = [], [], [], []
    left_slots = jnp.pad(weighted, ((0, TILE - BASIS), (0, 0)))
    expansions = jnp.zeros((TILE, TILE), F32)
    piece_message = ((PIECES, 24, TILE), F32)
    copied = ((PIECES * 17, TILE), F32)
    gene_message = ((PEERS, 3 * BLOCK, TILE), F32)
    for step in range(STEPS):
        position = BASIS + step * BLOCK
        if step == 0:
            message, raw, right_inverse, coeffs, combined, left_corr, slots, spare_slots, piece, rows, means8, stats = call(
                first_piece, "first_piece",
                [((PIECES * 18, TILE), F32), slim, slim, slim, slim, square, square, small, slim, small, small, small], arrived, basis_arrived, arrived=2)
        else:
            message, raw, coeffs, combined, piece, rows = call(
                later_piece, "piece", [copied, slim, slim, slim, slim, small],
                arrived, right_inverse, known, left_corr, slots, spare_slots, means8, stats, arrived=True)
        arrived = gather(message)
        factor, left_inverse, left_corr, slots, spare_slots = call(
            piece_state(position), "piece_state", [slim, slim, square, square, small],
            raw, right_inverse, coeffs, combined, left_corr, slots, spare_slots, piece, rows)
        diags.append(factor)
        if step == 0:
            (images,) = call(first_images, "first_images", [tall], image, stats, weights)
            block = images[BASIS : BASIS + BLOCK]
        left, left_slots = call(
            lambda a, b, c, d, position=position: new_left(a, b, c, d, position), "new_left", [wide, tall],
            block, combined, left_inverse, left_slots)
        lefts.append(left[:, :ROWS])
        arrived, left_inverse, left_corr, slots, spare_slots, images = lax.optimization_barrier(
            (arrived, left_inverse, left_corr, slots, spare_slots, images))
        if step == 0:
            message, genes_block, mean = call(first_genes, "first_genes", [gene_message, long, row],
                                              arrived, core_index, weights, *bases, streams=matrix, arrived=True, late_args=True)
        elif step + 1 < STEPS:
            message, genes_block = call(later_genes, "genes", [gene_message, long],
                                        arrived, mean, core_index, weights, *bases, streams=matrix, arrived=True, late_args=True)
        else:
            message, genes_block = call(last_genes, "last_genes", [((PEERS, BLOCK, TILE), F32), long],
                                        arrived, *bases, arrived=True)
        arrived = near(message)
        if step + 1 < STEPS:
            message, raw, coeffs, combined, block = call(
                later_cells, "cells", [piece_message, slim, slim, slim, wide],
                arrived, left_inverse, right_corr, images, weights, weighted, stats, streams=matrix, arrived=True)
            arrived = far(message)
            factor, right_inverse, known, right_corr, images, expansions, block = call(
                cells_state(position + BLOCK), "cells_state", [slim, slim, slim, square, tall, square, wide],
                raw, left_inverse, coeffs, combined, right_corr, images, expansions, block)
        else:
            both = all_genes(genes_block, partner(genes_block), core)
            right_vectors, couple_blocks = call(
                last_step, "last_step", [((STEPS * BLOCK, 2 * MAIN + TILE), F32), ((STEPS, BLOCK, BLOCK), F32)],
                arrived, left_inverse, right_corr, *couples, both, right_basis, right_start, *rights, arrived=True)
            break
        couples.append(factor)
        value, pair = call(new_right, "new_right", [long, ((2 * BLOCK, LOCAL), BF16)],
                           genes_block, left_inverse, combined, right_inverse, *bases)
        bases = bases + [pair]
        rights.append(all_genes(value, partner(value), core))
    left_vectors = jnp.concatenate(lefts, axis=0) * math.sqrt(8192.0)
    return left_vectors, right_vectors, jnp.stack([d[:, :BLOCK] for d in diags]), couple_blocks


def solution(mesh):
    split = Mesh(mesh.devices.reshape(8, 4, 2, 4), ("z", "y", "core", "x"))
    cells = ("z", "y", "core")
    return jax.shard_map(
        body,
        mesh=split,
        in_specs=(P(cells, "x"), P(cells), P(None, cells), P(None, "x"), P(None, "x")),
        out_specs=(P(None, cells), P(None, "x"), P(), P()),
        check_vma=False,
    )
```

```python
import inspect
import math

import jax
import jax.numpy as jnp
from jax import lax
from jax.experimental import pallas as pl
from jax.experimental.pallas import tpu as pltpu
from jax.sharding import Mesh
from jax.sharding import PartitionSpec as P

BASIS = 32
BLOCK = 16
STEPS = 3
ROWS = 128
TILE = 128
PIECES = 32
PEERS = 8
MAIN = PIECES * TILE
LOCAL = MAIN + TILE
CHUNKS = 3
SMALL = 50000
CHUNK = LOCAL // CHUNKS
HALF = TILE // 2
FAR = ("z", "y")
NEAR = ("core", "x")
F32 = jnp.float32
BF16 = jnp.bfloat16


def in_hbm(value):
    return pltpu.with_memory_space_constraint(value, pltpu.HBM)


def is_small(shape):
    return math.prod(shape) <= SMALL


def call(fn, name, outs, *args, streams=(), arrived=False, late_args=False):
    held = [is_small(a.shape) or n < int(arrived) for n, a in enumerate(args)]
    args = [a if h else in_hbm(a) for a, h in zip(args, held)]
    whole = list(streams[:1])
    streams = [in_hbm(a) for a in streams[1:]]
    count, kept, given = len(args), len(streams), len(outs)
    first = len(whole)
    loaded = [n for n in range(count) if not held[n]]
    stored = [n for n in range(given) if not is_small(outs[n][0])]
    total = len(loaded) + 2 * len(stored) + kept * CHUNKS

    def kernel(*refs):
        operands = refs[:count]
        resident = refs[count : count + first]
        sources = refs[count + first : count + first + kept]
        results = refs[count + first + kept : count + first + kept + given]
        scratch = refs[count + first + kept + given :]
        inside = scratch[: len(loaded)]
        written = scratch[len(loaded) : len(loaded) + len(stored)]
        parts = scratch[len(loaded) + len(stored) : len(loaded) + len(stored) + kept]
        semaphores = scratch[-1] if total else None
        entering = [pltpu.make_async_copy(operands[n], inside[m], semaphores.at[m]) for m, n in enumerate(loaded)]
        base = len(loaded) + 2 * len(stored)
        streaming = []
        for k in range(CHUNKS):
            window = (slice(None), pl.ds(k * CHUNK, CHUNK))
            streaming.append([
                pltpu.make_async_copy(source.at[window], parts[n].at[window], semaphores.at[base + n * CHUNKS + k])
                for n, source in enumerate(sources)
            ])
        first_copies = [copy for group in streaming for copy in group]
        for copy in first_copies + entering if late_args else entering + first_copies:
            copy.start()

        def chunk(k):
            for copy in streaming[k]:
                copy.wait()
            return [ref[:, k * CHUNK : (k + 1) * CHUNK] for ref in (*resident, *parts)]

        def late(m):
            def get():
                entering[m].wait()
                return inside[m][...]
            return get

        values = [operands[n][...] if held[n] else late(loaded.index(n)) for n in range(count)]
        leaving = []
        made = fn(*values, chunk) if kept else fn(*values)
        for n, value in made if inspect.isgenerator(made) else enumerate(made):
            if n not in stored:
                results[n][...] = value
                continue
            place = written[stored.index(n)]
            begin, value = value if isinstance(value, tuple) else (0, value)
            window = pl.ds(begin, value.shape[0])
            place[begin : begin + value.shape[0]] = value
            semaphore = semaphores.at[len(loaded) + 2 * stored.index(n) + (begin > 0)]
            copy = pltpu.make_async_copy(place.at[window], results[n].at[window], semaphore)
            copy.start()
            leaving.append(copy)
        for copy in leaving:
            copy.wait()

    vmem = pl.BlockSpec(memory_space=pltpu.VMEM)
    hbm = pl.BlockSpec(memory_space=pltpu.HBM)
    scratch_shapes = [pltpu.VMEM(args[n].shape, args[n].dtype) for n in loaded]
    scratch_shapes += [pltpu.VMEM(*outs[n]) for n in stored]
    scratch_shapes += [pltpu.VMEM(a.shape, a.dtype) for a in streams]
    if total:
        scratch_shapes.append(pltpu.SemaphoreType.DMA((total,)))
    return pl.pallas_call(
        kernel,
        out_shape=[pltpu.HBM(s, d) if n in stored else jax.ShapeDtypeStruct(s, d) for n, (s, d) in enumerate(outs)],
        in_specs=[vmem if h else hbm for h in held] + [vmem] * first + [hbm] * kept,
        out_specs=[hbm if n in stored else vmem for n in range(given)],
        scratch_shapes=scratch_shapes,
        compiler_params=pltpu.CompilerParams(vmem_limit_bytes=32 * 1024 * 1024),
        name=name,
    )(*args, *whole, *streams)


def roll(value, shift, axis):
    size = value.shape[axis]
    return pltpu.roll(value, shift % size, axis)


def mm(lhs, rhs):
    return lax.dot_general(lhs, rhs, (((1,), (0,)), ((), ())), precision=lax.Precision.HIGHEST, preferred_element_type=F32)


def mt(lhs, rhs):
    return lax.dot_general(lhs, rhs, (((1,), (1,)), ((), ())), precision=lax.Precision.HIGHEST, preferred_element_type=F32)


def tm(lhs, rhs):
    return lax.dot_general(lhs, rhs, (((0,), (0,)), ((), ())), precision=lax.Precision.HIGHEST, preferred_element_type=F32)


def two(value):
    high = value.astype(BF16)
    return jnp.concatenate([high, (value - high.astype(F32)).astype(BF16)], axis=0)


def folded(value):
    half = value.shape[0] // 2
    return value[:half] + value[half:]


def fine_mt(pair, high, low):
    dims = (((1,), (1,)), ((), ()))
    return folded(
        lax.dot_general(pair, high, dims, preferred_element_type=F32)
        + lax.dot_general(pair, low, dims, preferred_element_type=F32)
    )


def fine_mm(pair, high, low):
    dims = (((1,), (0,)), ((), ()))
    return folded(
        lax.dot_general(pair, high, dims, preferred_element_type=F32)
        + lax.dot_general(pair, low, dims, preferred_element_type=F32)
    )


def stream_mt(pair, chunk):
    dims = (((1,), (1,)), ((), ()))
    total = None
    for k in range(CHUNKS):
        part = pair[:, k * CHUNK : (k + 1) * CHUNK]
        for matrix in chunk(k):
            one = lax.dot_general(part, matrix, dims, preferred_element_type=F32)
            total = one if total is None else total + one
    return folded(total)


def stream_mm(pair, chunk):
    dims = (((1,), (0,)), ((), ()))
    parts = []
    for k in range(CHUNKS):
        high, low = chunk(k)
        parts.append(
            folded(
                lax.dot_general(pair, high, dims, preferred_element_type=F32)
                + lax.dot_general(pair, low, dims, preferred_element_type=F32)
            )
        )
    return jnp.concatenate(parts, axis=1)


def zeros(rows, lanes=TILE, dtype=F32):
    return jnp.zeros((rows, lanes), dtype)


def at_rows(value, start, rows=TILE):
    count, lanes = value.shape
    parts = []
    if start:
        parts.append(zeros(start, lanes, value.dtype))
    parts.append(value)
    if start + count < rows:
        parts.append(zeros(rows - start - count, lanes, value.dtype))
    return jnp.concatenate(parts, axis=0)


def lanes_of(shape):
    return lax.broadcasted_iota(jnp.int32, shape, 1)


def rows_of(shape):
    return lax.broadcasted_iota(jnp.int32, shape, 0)


def lane_range(value, start, stop):
    lane = lanes_of(value.shape)
    return jnp.where((lane >= start) & (lane < stop), value, 0.0)


def widened(value):
    return jnp.concatenate([value, zeros(value.shape[0], TILE - value.shape[1])], axis=1)


def factored(squares):
    lane = lanes_of((BLOCK, TILE))
    row = rows_of((BLOCK, TILE))
    work = squares + jnp.where(lane == row + BLOCK, 1.0, 0.0)
    factor = jnp.zeros((BLOCK, TILE), F32)
    for k in range(BLOCK):
        column = jnp.broadcast_to(work[:, k : k + 1], (BLOCK, TILE))
        scale = 1.0 / jnp.sqrt(jnp.broadcast_to(column[k : k + 1], (BLOCK, TILE)))
        column = column * scale
        pivot = work[k : k + 1] * scale
        factor = jnp.where((lane == k) & (row >= k), column, factor)
        work = jnp.where(row > k, work - column * pivot, jnp.where(row == k, pivot, work))
    return factor, lane_range(work, BLOCK, 2 * BLOCK)


def combination(coeffs, correlations):
    return coeffs + coeffs - mm(coeffs, correlations)


def scaled(raw, inverse):
    inner = inverse[:, :BLOCK]
    return widened(mt(mm(inner, raw[:, :BLOCK]), inner))


def orthonormal(coeffs, combined, squares, correlations, position):
    passed = mm(combined, correlations)
    remaining = squares + widened(mt(passed - coeffs, combined) - mt(combined, coeffs))
    factor, shifted = factored(remaining)
    inverse = lane_range(roll(shifted, -BLOCK, 1), 0, BLOCK)
    residual = mm(inverse[:, :BLOCK], coeffs - passed)
    identity = jnp.where(lanes_of((BLOCK, TILE)) == rows_of((BLOCK, TILE)) + position, 1.0, 0.0)
    full = residual + identity
    if position + BLOCK <= TILE:
        placed = at_rows(residual, position)
        correlations = correlations + placed + placed.T + at_rows(identity, position)
    return factor, inverse, full, correlations


def tiles(value, start, rows):
    return [value[start : start + rows, p * TILE : (p + 1) * TILE] for p in range(PIECES)]


def near_blocks(parts, core):
    blocks = []
    for target in range(2):
        same = core[0, 0] == target
        rows = []
        for a, b in parts:
            if b is None:
                rows.append(a)
            else:
                rows += [jnp.where(same, a, b), jnp.where(same, b, a)]
        blocks.append(jnp.concatenate(rows, axis=0))
    return blocks


def near_message(parts, core):
    blocks = near_blocks(parts, core)
    return jnp.stack([blocks[n // (PEERS // 2)] for n in range(PEERS)])


def halves(value):
    return value[:, :TILE], value[:, TILE:]


def start_kernel(tied, basis, block, chunk):
    lead = two(jnp.concatenate([basis(), block()], axis=0))
    yield 2, lead
    image = stream_mt(lead, chunk)
    count = BASIS + BLOCK
    gram = fine_mt(lead, jnp.concatenate([lead[:count], jnp.zeros((TILE - count, LOCAL), BF16)], axis=0),
                   jnp.concatenate([lead[count:], jnp.zeros((TILE - count, LOCAL), BF16)], axis=0))
    own, other = halves(image)
    yield 0, jnp.concatenate([own, other, gram], axis=0)
    yield 1, jnp.concatenate([other, own, gram], axis=0)


def basis_cells(weights, left_basis, chunk):
    weight = weights[:1]
    weighted = left_basis * weight
    ones = jnp.broadcast_to(weight, (8, weight.shape[1]))
    sums = mt(ones, jnp.concatenate([weighted, zeros(48, 2 * TILE), ones, zeros(TILE - 88, 2 * TILE)], axis=0))
    live = jnp.sum(weight, axis=1, keepdims=True)
    centred = weighted - jnp.sum(weighted, axis=1, keepdims=True) / live * weight
    lead = jnp.concatenate([centred, zeros(BLOCK, 2 * TILE), ones, zeros(8, 2 * TILE)], axis=0)
    product = stream_mm(two(lead), chunk)
    spare = jnp.concatenate([product[:, MAIN:], zeros(TILE - 64)], axis=0).T
    gram = mt(weighted, at_rows(weighted, 0))
    folds = gram[:8]
    for n in range(1, 4):
        folds = folds + roll(gram[8 * n : 8 * n + 8], BASIS * n, 1)
    row = rows_of((8, TILE))
    pieces = []
    for p in range(PIECES):
        main = product[:, p * TILE : (p + 1) * TILE]
        tail = jnp.where(row == 0, main[48:56], 0.0)
        tail = jnp.where(row == 1, spare[p : p + 1], tail)
        tail = jnp.where(row == 2, spare[PIECES + p : PIECES + p + 1], tail)
        tail = jnp.where(row == 3, sums, tail)
        pieces.append(jnp.concatenate([main[:BASIS], tail, folds], axis=0))
    return jnp.stack(pieces), weighted


def block_message(product, gram, rows):
    spare = at_rows(product[:, MAIN:], 48).T
    row8 = rows_of((8, TILE))
    tile = gram[:8] + roll(gram[8:], HALF, 1) + rows
    pieces = []
    for p in range(PIECES):
        tail = tile + jnp.where(row8 == 0, spare[p : p + 1], jnp.where(row8 == 1, spare[PIECES + p : PIECES + p + 1], 0.0))
        pieces.append(jnp.concatenate([product[:, p * TILE : (p + 1) * TILE], tail], axis=0))
    return jnp.stack(pieces)


def first_cells(arrived, weights, weighted, chunk):
    total = jnp.sum(arrived, axis=0)
    count = BASIS + BLOCK
    image = jnp.concatenate([total[:count], total[count : 2 * count]], axis=1)
    correlations = at_rows(total[2 * count :], 0)
    weight = weights[:1]
    block = image[BASIS:]
    ones = jnp.broadcast_to(weight, (8, weight.shape[1]))
    row8 = rows_of((8, TILE))
    rows = jnp.where(row8 == 2, mt(ones, at_rows(block, 48)), 0.0)
    for n in range(2):
        rows = rows + jnp.where(row8 == 3 + n, mt(ones, at_rows(image[BLOCK * n : BLOCK * n + BLOCK], 48)), 0.0)
    live = jnp.sum(weight, axis=1, keepdims=True)
    centred = block - jnp.sum(block, axis=1, keepdims=True) / live * weight
    gram = mt(centred, jnp.concatenate([weighted, centred, zeros(80, 2 * TILE)], axis=0))
    return block_message(stream_mm(two(centred), chunk), gram, rows), image, correlations


def copies(block):
    return jnp.concatenate([block] * PIECES, axis=0)


def cleaned_piece(main, spare, combined, slots, spare_slots):
    return main - mm(combined, slots), widened(spare[:, :BLOCK] - mt(spare_slots, combined))


def spare_line(rows):
    return rows[:1] + roll(rows[1:2], BASIS, 1)


def piece_state(position):
    def fn(raw, before, coeffs, combined, correlations, slots, spare_slots, piece, rows):
        squares = scaled(raw, before)
        factor, inverse, _, correlations = orthonormal(coeffs, combined, squares, correlations, position)
        inner = inverse[:, :BLOCK]
        slots = slots + at_rows(mm(inner, piece), position)
        spare_slots = spare_slots + roll(widened(mt(rows[:, :BLOCK], inner)), position, 1)
        return factor, inverse, correlations, slots, spare_slots
    return fn


def first_piece(arrived, basis_arrived):
    total = jnp.sum(arrived, axis=0)
    basis_total = jnp.sum(basis_arrived, axis=0)
    tile = total[BLOCK:]

    def moved(value):
        return roll(lane_range(value, 48, 64), -BLOCK, 1)

    sums = basis_arrived[:, 35, :] + moved(arrived[:, 18, :])
    shifted = moved(tile)
    every = basis_total[35:36] + shifted[2:3]
    images_sum = lane_range(tile, 48, 64)[3:4] + roll(lane_range(tile, 48, 64), BLOCK, 1)[4:5]
    lane = lanes_of(sums.shape)
    live = jnp.broadcast_to(sums[:, 80:81], sums.shape)
    whole = jnp.broadcast_to(every[:, 80:81], every.shape)
    scale = lax.rsqrt(whole)
    means = sums / live
    block_lane = (lane >= BASIS) & (lane < BASIS + BLOCK)
    weights = jnp.where(block_lane, means - every / whole, jnp.where(lane < BASIS, means, 0.0))
    column_mean = basis_total[32:33] / whole
    spread = basis_arrived[:, 32, :] - live * column_mean
    main = jnp.concatenate([basis_total[:BASIS], total[:BLOCK]], axis=0) + tm(weights, spread)[:48]
    spare = []
    spare_mean = []
    for k in range(2):
        mean = jnp.broadcast_to(basis_total[33 + k : 34 + k, 48:49], (1, TILE)) / whole
        column = jnp.broadcast_to(basis_arrived[:, 33 + k, 48:49], sums.shape) - live * mean
        known = lane_range(basis_total[33 + k : 34 + k], 0, BASIS) + shifted[k : k + 1]
        spare.append(known + jnp.sum(weights * column, axis=0, keepdims=True))
        spare_mean.append(mean)
    gram = jnp.concatenate([tile, roll(tile, -HALF, 1)], axis=0)
    between = tm(weights, jnp.where(lane < BASIS, sums, live * weights))[BASIS : BASIS + BLOCK]
    inner = gram + between
    scale16 = jnp.broadcast_to(scale, (BLOCK, TILE))
    coeffs = lane_range(inner, 0, BASIS) * scale16
    squares = lane_range(roll(inner, -BASIS, 1), 0, BLOCK) * scale16 * scale16
    folds = basis_total[40:48]
    basis_gram = jnp.concatenate([lane_range(roll(folds, -BASIS * n, 1), 0, BASIS) for n in range(4)], axis=0)
    correlations = at_rows(basis_gram, 0)
    combined = combination(coeffs, correlations)
    row8 = rows_of((8, TILE))
    both = lane_range(jnp.where(row8 == 0, spare[0], jnp.where(row8 == 1, spare[1], 0.0)), 0, 48) * scale
    slots = at_rows(main[:BASIS] * jnp.broadcast_to(scale, (BASIS, TILE)), 0)
    spare_slots = lane_range(both, 0, BASIS)
    block_main = main[BASIS:] * scale16 * scale16
    block_spare = lane_range(roll(both, -BASIS, 1), 0, BLOCK) * scale
    piece, rows = cleaned_piece(block_main, block_spare, combined, slots, spare_slots)
    lane1 = lanes_of((1, TILE))
    tail = spare_line(rows)
    for k in range(2):
        tail = jnp.where(lane1 == BASIS * k + BLOCK, spare_mean[k], tail)
    means8 = jnp.where(row8 == 0, column_mean, jnp.where(row8 == 1, spare_mean[0], jnp.where(row8 == 2, spare_mean[1], 0.0)))
    stats = jnp.where(row8 == 0, scale, jnp.where(row8 == 1, (every + images_sum) / whole, 0.0))
    message = copies(jnp.concatenate([piece, tail, column_mean], axis=0))
    before = jnp.where(lanes_of((BLOCK, TILE)) == rows_of((BLOCK, TILE)), 1.0, 0.0)
    return message, squares, before, coeffs, combined, correlations, slots, spare_slots, piece, rows, means8, stats


def later_piece(arrived, inverse, known, correlations, slots, spare_slots, means8, stats):
    total = jnp.sum(arrived, axis=0)
    inner = inverse[:, :BLOCK]
    tile = total[BLOCK:]
    gram = jnp.concatenate([tile, roll(tile, -HALF, 1)], axis=0)
    coeffs = mm(inner, lane_range(gram, 0, BASIS)) + known
    squares = lane_range(roll(gram, -BASIS, 1), 0, BLOCK)
    combined = combination(coeffs, correlations)
    scale = stats[:1]
    rows = widened(mt(roll(tile, -48, 1)[:, :BLOCK], inner))
    row8 = rows_of((8, TILE))
    sums = jnp.broadcast_to(rows[2:3], (8, TILE))
    outer = tm(jnp.where(row8 == 0, sums, 0.0), jnp.where(row8 == 0, jnp.broadcast_to(means8[:1], (8, TILE)), 0.0))[:BLOCK]
    main = (mm(inner, total[:BLOCK]) - outer) * jnp.broadcast_to(scale, (BLOCK, TILE))
    spare_mean = jnp.where(row8 == 0, means8[1:2], jnp.where(row8 == 1, means8[2:3], 0.0))
    spare = jnp.where(row8 < 2, (rows - sums * spare_mean) * scale, 0.0)
    piece, fresh = cleaned_piece(main, spare, combined, slots, spare_slots)
    fresh = jnp.where(row8 < 2, fresh, 0.0)
    message = copies(jnp.concatenate([piece, spare_line(fresh)], axis=0))
    return message, squares, coeffs, combined, piece, fresh


def gathered(arrived):
    size = arrived.shape[0] // PIECES
    lines = jnp.concatenate([arrived[p * size + BLOCK : p * size + BLOCK + 1] for p in range(PIECES)], axis=0)
    spare = jnp.concatenate([lines, roll(lines, -BASIS, 1), zeros(TILE - 2 * PIECES)], axis=0).T
    block = jnp.concatenate(
        [arrived[p * size : p * size + BLOCK] for p in range(PIECES)] + [lane_range(spare[:BLOCK], 0, HALF)], axis=1)
    return block, spare


def gene_gram(pair, mean, bases):
    mean_pair = two(jnp.broadcast_to(mean, (BLOCK, LOCAL)))
    bases = [b() for b in bases]
    known = sum(b.shape[0] // 2 for b in bases)
    gap = jnp.zeros((80 - known, LOCAL), BF16)
    end = jnp.zeros((BLOCK, LOCAL), BF16)
    tops = [b[: b.shape[0] // 2] for b in bases] + ([gap] if known < 80 else []) + [pair[:BLOCK], mean_pair[:BLOCK], end]
    lows = [b[b.shape[0] // 2 :] for b in bases] + ([gap] if known < 80 else []) + [pair[BLOCK:], mean_pair[BLOCK:], end]
    return fine_mt(pair, jnp.concatenate(tops, axis=0), jnp.concatenate(lows, axis=0))


def gene_sums(pair, mean, core, weights, bases, chunk):
    image = stream_mt(pair, chunk)
    gram = gene_gram(pair, mean, bases)
    image = image - gram[:, 96:97] * weights[:1]
    return near_message([halves(image), (lane_range(gram, 0, 96), None)], core)


def first_genes(arrived, core, weights, *rest):
    block, spare = gathered(arrived)
    yield 1, block
    mean = jnp.concatenate(
        [arrived[18 * p + 17 : 18 * p + 18] for p in range(PIECES)] + [lane_range(spare[BLOCK : BLOCK + 1], 0, HALF)], axis=1)
    yield 2, mean
    yield 0, gene_sums(two(block), mean, core, weights, rest[:-1], rest[-1])


def later_genes(arrived, mean, core, weights, *rest):
    block, _ = gathered(arrived)
    yield 1, block
    yield 0, gene_sums(two(block), mean, core, weights, rest[:-1], rest[-1])


def last_genes(arrived, *bases):
    block, _ = gathered(arrived)
    yield 1, block
    gram = lane_range(gene_gram(two(block), zeros(1, LOCAL), bases), 0, 96)
    yield 0, jnp.stack([gram] * PEERS)


def later_cells(arrived, before, correlations, images, weights, weighted, stats, chunk):
    total = jnp.sum(arrived, axis=0)
    inner = before[:, :BLOCK]
    image = mm(inner, jnp.concatenate([total[:BLOCK], total[BLOCK : 2 * BLOCK]], axis=1))
    gram = total[2 * BLOCK :]
    coeffs = mm(inner, lane_range(gram, 0, 80))
    squares = lane_range(roll(gram, -80, 1), 0, BLOCK)
    combined = combination(coeffs, correlations)
    block = image * stats[:1, :1] - mm(combined, images)
    sums = mt(jnp.broadcast_to(weights[:1], (8, 2 * TILE)), at_rows(block, 48))
    gram = mt(block, jnp.concatenate([weighted, block, zeros(80, 2 * TILE)], axis=0))
    rows = jnp.where(rows_of((8, TILE)) == 2, sums, 0.0)
    return block_message(stream_mm(two(block), chunk), gram, rows), squares, coeffs, combined, block


def cells_state(position):
    def fn(raw, before, coeffs, combined, correlations, images, expansions, block):
        squares = scaled(raw, before)
        factor, inverse, full, correlations = orthonormal(coeffs, combined, squares, correlations, position)
        block = mm(inverse[:, :BLOCK], block)
        images = images + at_rows(block, position)
        expansions = expansions + at_rows(combined + roll(factor, position, 1), position - BLOCK)
        return factor, inverse, mt(full, expansions), correlations, images, expansions, block
    return fn


def last_step(arrived, before, correlations, first_factor, second_factor, block, basis, start, first, second):
    size = math.sqrt(33280.0)
    gram = jnp.sum(arrived, axis=0)
    coeffs = mm(before[:, :BLOCK], lane_range(gram, 0, 80))
    squares = scaled(roll(gram, -80, 1), before)
    combined = combination(coeffs, correlations)
    factor, inverse, _, _ = orthonormal(coeffs, combined, squares, correlations, BASIS + STEPS * BLOCK)
    inner = inverse[:, :BLOCK]
    first, second = first(), second()
    yield 0, (0, jnp.concatenate([first, second], axis=0) * size)
    slots = jnp.concatenate([basis(), start(), first, second], axis=0)
    high = slots.astype(BF16)
    low = (slots - high.astype(F32)).astype(BF16)
    value = mm(mm(inner, before[:, :BLOCK]), block()) - fine_mm(two(mm(inner, combined)[:, :80]), high, low)
    yield 0, (2 * BLOCK, value * size)
    yield 1, jnp.stack([first_factor[:, :BLOCK], second_factor[:, :BLOCK], factor[:, :BLOCK]])


def first_images(image, stats, weights):
    scale = stats[:1, :1]
    both = image
    means = stats[1:2]
    means = jnp.concatenate([means[:, 48:80], means[:, BASIS : BASIS + BLOCK]], axis=1)
    column = at_rows(widened(jnp.broadcast_to(means, (8, 48))), 0).T[:48, :1]
    return (at_rows((both - column * weights[:1]) * scale, 0),)


def new_right(block, before, combined, inverse, *bases):
    bases = [b() for b in bases]
    known = sum(b.shape[0] // 2 for b in bases)
    high = jnp.concatenate([b[: b.shape[0] // 2] for b in bases], axis=0)
    low = jnp.concatenate([b[b.shape[0] // 2 :] for b in bases], axis=0)
    inner = inverse[:, :BLOCK]
    value = mm(mm(inner, before[:, :BLOCK]), block()) - fine_mm(two(mm(inner, combined)[:, :known]), high, low)
    return value, two(value)


def new_left(block, combined, inverse, slots, position):
    value = mm(inverse[:, :BLOCK], block - mm(combined, slots))
    return value, slots + at_rows(value, position)


def gather(value):
    size = value.shape[0] // PIECES * TILE
    return far(value.reshape(PIECES, 1, size)).reshape(value.shape)


def far(value):
    return lax.all_to_all(value, FAR, split_axis=0, concat_axis=0, tiled=True)


def near(value):
    return lax.all_to_all(value, NEAR, split_axis=0, concat_axis=0, tiled=True)


def partner(value):
    return lax.ppermute(value, "core", [(0, 1), (1, 0)])


def own_genes(value, core):
    main = lax.dynamic_slice_in_dim(value, core * MAIN, MAIN, 1)
    spare = jnp.where(core == 0, value[:, 2 * MAIN : 2 * MAIN + HALF], value[:, 2 * MAIN + HALF :])
    return jnp.concatenate([main, jnp.pad(spare, ((0, 0), (0, HALF)))], axis=1)


def all_genes(own, other, core):
    first = jnp.where(core == 0, own, other)
    second = jnp.where(core == 0, other, own)
    return jnp.concatenate([first[:, :MAIN], second[:, :MAIN], first[:, MAIN : MAIN + HALF], second[:, MAIN : MAIN + HALF]], axis=1)


def body(counts, live_rows, left_basis, right_basis, right_start):
    core = lax.axis_index("core")
    core_index = jnp.full((8, TILE), core, jnp.int32)
    live = live_rows[0]
    sent = own_genes(counts, 1 - core)
    got = partner(sent)
    cells = jnp.arange(ROWS, dtype=jnp.int32)
    weight = (cells < live).astype(F32)
    bundle = jnp.concatenate([left_basis, jnp.broadcast_to(weight, (8, ROWS))], axis=0)
    got_bundle = partner(bundle)
    weights = jnp.concatenate([bundle[BASIS:], got_bundle[BASIS:]], axis=1)
    basis_left = jnp.concatenate([left_basis, got_bundle[:BASIS]], axis=1)
    every = jnp.concatenate([own_genes(counts, core), got], axis=0)
    logged = jnp.where(weights[0][:, None] > 0, jnp.log(1.0 + every.astype(F32)), 0.0)
    top = lax.reduce_precision(logged, 8, 7)
    high, low = top.astype(BF16), (logged - top).astype(BF16)
    basis_right = own_genes(right_basis, core)
    start = own_genes(right_start, core)

    square = ((TILE, TILE), F32)
    slim = ((BLOCK, TILE), F32)
    small = ((8, TILE), F32)
    wide = ((BLOCK, 2 * TILE), F32)
    tall = ((TILE, 2 * TILE), F32)
    long = ((BLOCK, LOCAL), F32)
    row = ((1, LOCAL), F32)
    count = BASIS + BLOCK

    matrix = (high, low)
    basis_message, weighted = call(
        basis_cells, "basis_cells", [((PIECES, 48, TILE), F32), ((BASIS, 2 * TILE), F32)],
        weights, basis_left, streams=matrix)
    basis_arrived = far(basis_message)
    basis_message, tied = lax.optimization_barrier((basis_message, weights))
    own_sums, other_sums, lead = call(
        start_kernel, "start", [((3 * count, TILE), F32), ((3 * count, TILE), F32), ((2 * count, LOCAL), BF16)],
        tied, basis_right, start, streams=matrix)
    bases = [lead]
    chip_sums = own_sums + partner(other_sums)
    arrived = jnp.stack([chip_sums] + [lax.ppermute(chip_sums, "x", [(i, (i + k) % 4) for i in range(4)]) for k in (1, 2, 3)])
    message, image, right_corr = call(
        first_cells, "first_cells", [((PIECES, 24, TILE), F32), ((count, 2 * TILE), F32), square],
        arrived, weights, weighted, streams=matrix, arrived=True)
    message, basis_arrived = lax.optimization_barrier((message, basis_arrived))
    arrived = far(message)
    lefts, rights, diags, couples = [], [], [], []
    left_slots = jnp.pad(weighted, ((0, TILE - BASIS), (0, 0)))
    expansions = jnp.zeros((TILE, TILE), F32)
    piece_message = ((PIECES, 24, TILE), F32)
    copied = ((PIECES * 17, TILE), F32)
    gene_message = ((PEERS, 3 * BLOCK, TILE), F32)
    for step in range(STEPS):
        position = BASIS + step * BLOCK
        if step == 0:
            message, raw, right_inverse, coeffs, combined, left_corr, slots, spare_slots, piece, rows, means8, stats = call(
                first_piece, "first_piece",
                [((PIECES * 18, TILE), F32), slim, slim, slim, slim, square, square, small, slim, small, small, small], arrived, basis_arrived, arrived=2)
        else:
            message, raw, coeffs, combined, piece, rows = call(
                later_piece, "piece", [copied, slim, slim, slim, slim, small],
                arrived, right_inverse, known, left_corr, slots, spare_slots, means8, stats, arrived=True)
        arrived = gather(message)
        factor, left_inverse, left_corr, slots, spare_slots = call(
            piece_state(position), "piece_state", [slim, slim, square, square, small],
            raw, right_inverse, coeffs, combined, left_corr, slots, spare_slots, piece, rows)
        diags.append(factor)
        if step == 0:
            (images,) = call(first_images, "first_images", [tall], image, stats, weights)
            block = images[BASIS : BASIS + BLOCK]
        left, left_slots = call(
            lambda a, b, c, d, position=position: new_left(a, b, c, d, position), "new_left", [wide, tall],
            block, combined, left_inverse, left_slots)
        lefts.append(left[:, :ROWS])
        state = (arrived, left_inverse, left_corr, slots, spare_slots, images)
        if step + 1 == STEPS:
            left_vectors = jnp.concatenate(lefts, axis=0) * math.sqrt(8192.0)
            diag_blocks = jnp.stack([d[:, :BLOCK] for d in diags])
            *state, left_vectors, diag_blocks = lax.optimization_barrier((*state, left_vectors, diag_blocks))
        else:
            state = lax.optimization_barrier(state)
        arrived, left_inverse, left_corr, slots, spare_slots, images = state
        if step == 0:
            message, genes_block, mean = call(first_genes, "first_genes", [gene_message, long, row],
                                              arrived, core_index, weights, *bases, streams=matrix, arrived=True, late_args=True)
        elif step + 1 < STEPS:
            message, genes_block = call(later_genes, "genes", [gene_message, long],
                                        arrived, mean, core_index, weights, *bases, streams=matrix, arrived=True, late_args=True)
        else:
            message, genes_block = call(last_genes, "last_genes", [((PEERS, BLOCK, TILE), F32), long],
                                        arrived, *bases, arrived=True)
        arrived = near(message)
        if step + 1 < STEPS:
            message, raw, coeffs, combined, block = call(
                later_cells, "cells", [piece_message, slim, slim, slim, wide],
                arrived, left_inverse, right_corr, images, weights, weighted, stats, streams=matrix, arrived=True)
            arrived = far(message)
            factor, right_inverse, known, right_corr, images, expansions, block = call(
                cells_state(position + BLOCK), "cells_state", [slim, slim, slim, square, tall, square, wide],
                raw, left_inverse, coeffs, combined, right_corr, images, expansions, block)
        else:
            both = all_genes(genes_block, partner(genes_block), core)
            right_vectors, couple_blocks = call(
                last_step, "last_step", [((STEPS * BLOCK, 2 * MAIN + TILE), F32), ((STEPS, BLOCK, BLOCK), F32)],
                arrived, left_inverse, right_corr, *couples, both, right_basis, right_start, *rights, arrived=True)
            break
        couples.append(factor)
        value, pair = call(new_right, "new_right", [long, ((2 * BLOCK, LOCAL), BF16)],
                           genes_block, left_inverse, combined, right_inverse, *bases)
        bases = bases + [pair]
        rights.append(all_genes(value, partner(value), core))
    return left_vectors, right_vectors, diag_blocks, couple_blocks


def solution(mesh):
    split = Mesh(mesh.devices.reshape(8, 4, 2, 4), ("z", "y", "core", "x"))
    cells = ("z", "y", "core")
    return jax.shard_map(
        body,
        mesh=split,
        in_specs=(P(cells, "x"), P(cells), P(None, cells), P(None, "x"), P(None, "x")),
        out_specs=(P(None, cells), P(None, "x"), P(), P()),
        check_vma=False,
    )
```
